32 devices in a mesh: gx: 4 (over y, x), gy: 2 (over core), gz: 4 (over z).
Axes of the slice: x: 2, y: 2, z: 4, core: 2. Of those that a mesh axis runs over, the one named last changes fastest.
Arguments:
- right_side: float32 [81, 16, 16, 512], P(None, 'gx', 'gy', 'gz'), may hold values from -18 to 18
- cell_coef: float32 [16, 16, 128], P('gx', 'gy', 'gz'), may hold values from 0.5 to 2
- cell_matrix: float32 [81, 81], replicated, may hold values from -2 to 16, as said below
- face_coupling: float32 [3, 81, 81], replicated, may hold values from -0.18 to 0.18
- patch_inverse: bfloat16 [648, 648], replicated, may hold values from -0.01 to 0.1, as said below
Outputs:
- solution: float32 [81, 16, 16, 512], P(None, 'gx', 'gy', 'gz')
- residual: float32 [81, 16, 16, 512], P(None, 'gx', 'gy', 'gz')
The draws below stay inside these ranges and needn't reach their ends.
Inputs may be any that keep to these rules, and one draw needn't show every extreme that they name: `cell_matrix`: symmetric. `patch_inverse`: symmetric.
All inputs are finite; a program needn't handle non-finite values.
Results may differ from the reference program's by a relative error of at most 0.035.
Values may be sent and summed in bfloat16 or wider, within the bound.
A program may use at most 192 MiB of HBM per device.

```python
import math
import jax
import jax.numpy as jnp
from jax import lax

Q = 81
PATCH = 648
RHS = 4
NX = 16
NY = 16
NZ = 128


def symmetric_part(key, matrix_order):
    sampled = jnp.clip(jax.random.normal(key, (matrix_order, matrix_order), jnp.float32), -4.0, 4.0)
    return (sampled + sampled.T) * 0.7071


def draw_cell_matrix(key, part):
    key_diag = jax.random.fold_in(key, 11)
    key_rest = jax.random.fold_in(key, 12)
    diagonal = jax.random.uniform(key_diag, (Q,), jnp.float32, 10.8, 13.2)
    return jnp.diag(diagonal) + 0.35 * symmetric_part(key_rest, Q)


def draw_patch_inverse(key, part):
    key_diag = jax.random.fold_in(key, 21)
    key_rest = jax.random.fold_in(key, 22)
    diagonal = jax.random.uniform(key_diag, (PATCH,), jnp.float32, 0.9, 1.1)
    values = (jnp.diag(diagonal) + 0.012 * symmetric_part(key_rest, PATCH)) / 12.0
    return values.astype(jnp.bfloat16)


def shard_levels(stream_key, extent, split, low, largest):
    gain, own = 1.0, jax.random.fold_in(stream_key, 6)
    for position, parts in split:
        draws = jnp.exp(jax.random.uniform(jax.random.fold_in(own, position), (parts,), jnp.float32, low / len(split), largest / len(split)))
        gain = gain * jnp.repeat(draws, extent[position] // parts).reshape([-1 if axis == position else 1 for axis in range(len(extent))])
    return gain


def normal_values(key, dims, scale, limit, cuts=(), dtype=jnp.bfloat16):
    values = scale * jax.random.normal(key, dims, jnp.float32)
    if cuts:
        values = values * shard_levels(key, dims, cuts, -0.22, 0.18)
    return jnp.clip(values, -limit, limit).astype(dtype)


def setup_inputs(seed: int = 0) -> dict:
    keys = jax.random.split(jax.random.key(seed), 6)
    return {
        "right_side": normal_values(keys[0], (Q, NX, NY, NZ * RHS), 3.0, 18.0, ((1, 4), (2, 2), (3, 4)), jnp.float32),
        "cell_coef": jnp.clip(jnp.exp(math.log(2.0) - 1.3862944 * jax.random.uniform(keys[1], (NX, NY, NZ), jnp.float32) ** shard_levels(keys[1], (NX, NY, NZ), ((0, 4), (1, 2), (2, 4)), -0.2, 0.2)), 0.5, 2.0),
        "cell_matrix": draw_cell_matrix(jax.random.fold_in(keys[5], 71), 0),
        "face_coupling": normal_values(keys[3], (3, Q, Q), 0.03, 0.18, (), jnp.float32),
        "patch_inverse": draw_patch_inverse(jax.random.fold_in(keys[5], 71), 0),
    }


HIGH = lax.Precision.HIGHEST

def operator(values, cell_coef, cell_matrix, face_coupling):
    result = cell_coef[None, :, :, :, None] * jnp.einsum('pq,qxyzr->pxyzr', cell_matrix, values, precision=HIGH)
    for direction in range(3):
        forward = jnp.roll(values, -1, direction + 1)
        behind = jnp.roll(values, 1, direction + 1)
        result = result - jnp.einsum('pq,qxyzr->pxyzr', face_coupling[direction], forward, precision=HIGH)
        result = result - jnp.einsum('qp,qxyzr->pxyzr', face_coupling[direction], behind, precision=HIGH)
    return result

def reference(right_side, cell_coef, cell_matrix, face_coupling, patch_inverse):
    dof_count = cell_matrix.shape[0]
    residual = right_side.reshape(dof_count, NX, NY, NZ, RHS)
    solution = jnp.zeros_like(residual)
    scaling = lax.rsqrt(cell_coef)[None, :, :, :, None]
    blocks = patch_inverse.astype(jnp.float32).reshape(dof_count, 2, 2, 2, dof_count, 2, 2, 2)
    for colour in range(8):
        shifts = (1 - colour // 4, 1 - colour // 2 % 2, 1 - colour % 2)
        scaled = (scaling * residual).astype(jnp.bfloat16)
        scaled = lax.optimization_barrier(scaled).astype(jnp.float32)
        rolled = jnp.roll(scaled, shifts, axis=(1, 2, 3))
        blocked = rolled.reshape(dof_count, NX // 2, 2, NY // 2, 2, NZ // 2, 2, RHS)
        solved = jnp.einsum('qijkplmn,pXlYmZnr->qXiYjZkr', blocks, blocked, precision=HIGH)
        solved = solved.reshape(dof_count, NX, NY, NZ, RHS)
        solved = jnp.roll(solved, (-shifts[0], -shifts[1], -shifts[2]), axis=(1, 2, 3))
        correction = scaling * solved
        solution = solution + correction
        residual = residual - operator(correction, cell_coef, cell_matrix, face_coupling)
    return (solution.reshape(right_side.shape), residual.reshape(right_side.shape))
```

```python
import functools
import jax
import jax.numpy as jnp
from jax import lax
from jax.experimental import pallas as pl
from jax.experimental.pallas import tpu as pltpu
from jax.sharding import PartitionSpec as P

AXES = ("gx", "gy", "gz")
MESH = pl.DeviceIdType.MESH
F32, BF16 = jnp.float32, jnp.bfloat16
LANES = 128


def class_pairs(d):
    bit = 4 >> d
    return [(c, c + bit) for c in range(8) if not c & bit]


def block_kernel(sizes, dims, start_ref, inverse_ref, w_ref, sol_ref, res_ref,
           R, S2, Sx, scaled, corr, ccorr, Xx, Xy, Xz,
           fx, fxe, fy, fz, fxes, fys, fzs, mxr, mxe, mxs, myr, mys, mzr,
           mxr_s, mxs_s, myr_s, mys_s, mzr_s, p_rows, p_ref, send_sem, recv_sem):
    D, Q, nr, ni, njh = dims
    w = 2 * nr
    A = Q // 16 * 16
    tiles = [(i, jh) for i in range(ni) for jh in range(njh)]
    C = ni * njh * LANES
    half = njh * LANES
    lane = lax.broadcasted_iota(jnp.int32, (D, LANES), 1)
    jlo0 = (lane // nr) % 2 == 0
    piece = lane // w

    me = [lax.axis_index(a) for a in AXES]

    def neighbour(d, step):
        n = sizes[d]
        return {AXES[d]: lax.rem(me[d] + step + n, n)}

    barrier = pltpu.get_barrier_semaphore()
    for d in range(3):
        for step in (1, -1):
            pl.semaphore_signal(barrier, inc=1, device_id=neighbour(d, step), device_id_type=MESH)

    def rows(c):
        return slice(c * D, (c + 1) * D)

    def cols(i, jh):
        t = i * njh + jh
        return slice(t * LANES, (t + 1) * LANES)

    def get(ref, c):
        return {t: ref[c, :, cols(*t)].astype(F32) for t in tiles}

    def roll(x, s):
        s = s % LANES
        return pltpu.roll(x, s, 1) if s else x

    for c in range(0, 8, 2):
        ox, oy = c // 4, c // 2 % 2
        for i, jh in tiles:
            a = start_ref[2 * i + ox, 4 * jh + oy]
            b = start_ref[2 * i + ox, 4 * jh + 2 + oy]
            R[c, :, cols(i, jh)] = jnp.where(jlo0, a, roll(b, nr))
            R[c + 1, :, cols(i, jh)] = jnp.where(jlo0, roll(a, -nr), b)
    S2[...] = jnp.zeros_like(S2)
    pl.semaphore_wait(barrier, 6)

    def pack_y(ref, last):
        out = []
        for p in class_pairs(1):
            c = p[1] if last else p[0]
            jh = njh - 1 if last else 0
            t0 = ref[c, :, cols(0, jh)].astype(F32)
            t1 = ref[c, :, cols(1, jh)].astype(F32)
            if last:
                out.append(jnp.where(jlo0, roll(t1, -nr), t0))
            else:
                out.append(jnp.where(jlo0, t0, roll(t1, nr)))
        return jnp.stack(out, 0)

    def pack_z(ref, last):
        acc = jnp.zeros((D, LANES), F32)
        n = 0
        for p in class_pairs(2):
            c = p[1] if last else p[0]
            for t in tiles:
                x = ref[c, :, cols(*t)].astype(F32)
                x = roll(x, w * (n + 1) if last else w * n)
                acc = jnp.where(piece == n, x, acc)
                n += 1
        return acc

    def shifted(d, step, have, halo, pc):
        out = {}
        for i, jh in tiles:
            if d == 0:
                at = i + step
                if 0 <= at < ni:
                    new = have[at, jh]
                else:
                    new = halo(slice(jh * LANES, (jh + 1) * LANES))
            elif d == 1:
                at = jh + step
                if 0 <= at < njh:
                    other = roll(have[i, at], step * nr)
                else:
                    other = halo(slice(0, LANES))
                    if i == 0:
                        other = roll(other, step * nr)
                cur = roll(have[i, jh], -step * nr)
                new = jnp.where(jlo0, cur, other) if step == 1 else jnp.where(jlo0, other, cur)
            else:
                n = pc * len(tiles) + i * njh + jh
                h = halo(slice(0, LANES))
                if step == 1:
                    new = jnp.where(lane >= LANES - w, roll(h, LANES - w - w * n),
                                    roll(have[i, jh], -w))
                else:
                    new = jnp.where(lane < w, roll(h, -w * n), roll(have[i, jh], w))
            out[i, jh] = new
        return out

    def read_x(t, last, pc):
        first = lax.broadcasted_iota(jnp.int32, (D - A, LANES), 0) == 0

        def halo(c):
            tail = fxe[t, last, :, c].astype(F32)[pc:pc + 1]
            return jnp.concatenate(
                [fx[t, last, pc, :, c].astype(F32), jnp.where(first, tail, 0.0)], 0)
        return halo

    def read_y(ref, *at):
        return lambda c: ref[(*at, slice(None), c)].astype(F32)

    def remote(src, dst, k, d, step):
        return pltpu.make_async_remote_copy(
            src_ref=src, dst_ref=dst, send_sem=send_sem.at[k], recv_sem=recv_sem.at[k],
            device_id=neighbour(d, step), device_id_type=MESH)

    def move(d, down, copies, halo, beside=None):
        for copy in copies:
            copy.start()
        if beside is not None:
            beside()
        for copy in copies:
            copy.wait()
        for pc, (c0, c1) in enumerate(class_pairs(d)):
            old0, old1 = get(R, c0), get(R, c1)
            if down:
                new0, new1 = shifted(d, -1, old1, halo(pc), pc), old0
            else:
                new0, new1 = old1, shifted(d, 1, old0, halo(pc), pc)
            for t in tiles:
                R[c0, :, cols(*t)] = new0[t]
                R[c1, :, cols(*t)] = new1[t]

    def move_x(down, at, beside=None):
        part = slice((ni - 1) * half, ni * half) if down else slice(0, half)
        cs = slice(4, 8) if down else slice(0, 4)
        mxr_s[...] = R[cs, :A, part].astype(BF16)
        step = 1 if down else -1
        copies = [remote(mxr_s, mxr.at[at], 72 + at, 0, step),
                  remote(R.at[cs, A:A + 8, part], mxe.at[at], 74 + at, 0, step)]
        zeros = jnp.zeros((D - A - 8, LANES), F32)

        def halo(pc):
            return lambda c: jnp.concatenate(
                [mxr[at, pc, :, c].astype(F32), mxe[at, pc, :, c], zeros], 0)
        move(0, down, copies, halo, beside)

    def move_y(down, u):
        myr_s[...] = pack_y(R, down)
        move(1, down, [remote(myr_s, myr.at[u], 64 + u, 1, 1 if down else -1)],
             lambda pc: read_y(myr, u, pc))

    def move_z(down, t):
        mzr_s[...] = pack_z(R, down)
        move(2, down, [remote(mzr_s, mzr.at[t], 48 + t, 2, 1 if down else -1)],
             lambda pc: read_y(mzr, t))

    def sol_y(u):
        return remote(mys_s, mys.at[lax.div(u, 2)], 56 + lax.div(u, 2), 1, -1)

    def sol_x():
        return remote(mxs_s, mxs, 58, 0, -1)

    def pair(ref, q):
        return ref[2 * q:2 * q + 2].reshape(2 * D, C)

    def lessen(q, acc):
        R[2 * q:2 * q + 2] -= acc.reshape(2, D, C)

    def dot(a, b):
        return jnp.dot(a, b, preferred_element_type=F32)

    def colour(t, v, sb):
        for c in range(8):
            s = R[c, Q:Q + 1, :]
            scaled[c] = (s * R[c]).astype(BF16)
        copies = [[None, None] for _ in range(3)]
        extra = [None, None]
        line = lax.broadcasted_iota(jnp.int32, (16, half), 0)
        for n in range(ni):
            part = slice(n * half, (n + 1) * half)
            solved = dot(p_ref[...], scaled[:, :, part].reshape(8 * D, half))
            for c in range(8):
                s = R[c, Q:Q + 1, part]
                k = R[c, Q + 1:Q + 2, part]
                got = s * solved[rows(c), :]
                if v == 1:
                    S2[sb, c, :, part] += got
                corr[c, :, part] = got.astype(BF16)
                ccorr[c, :, part] = (k * got).astype(BF16)
            for last in (0, 1):
                if n != (ni - 1 if last else 0):
                    continue
                step = 1 if last else -1
                tail = jnp.zeros((16, half), F32)
                for pc in range(4):
                    row = corr[4 * last + pc, A:, part].astype(F32)[:1]
                    tail = jnp.where(line == pc, row, tail)
                fxes[last] = tail.astype(BF16)
                copies[0][last] = remote(corr.at[4 * last:4 * last + 4, :A, part], fx.at[t, last],
                                         t * 6 + last, 0, step)
                copies[0][last].start()
                extra[last] = remote(fxes.at[last], fxe.at[t, last], 80 + 2 * t + last, 0, step)
                extra[last].start()
        for last in (0, 1):
            fzs[last] = pack_z(corr, last).astype(BF16)
            copies[2][last] = remote(fzs.at[last], fz.at[t, last], t * 6 + 4 + last, 2, 1 if last else -1)
            copies[2][last].start()
        for last in (0, 1):
            fys[last] = pack_y(corr, last).astype(BF16)
            copies[1][last] = remote(fys.at[last], fy.at[t, last], t * 6 + 2 + last, 1, 1 if last else -1)
            copies[1][last].start()
        for q in range(4):
            acc = dot(w_ref[0], pair(ccorr, q))
            acc += dot(w_ref[1], pair(corr, q))
            acc += dot(w_ref[3 if q // 2 == 0 else 4], pair(corr, q ^ 2))
            acc += dot(w_ref[5 if q % 2 == 0 else 6], pair(corr, q ^ 1))
            lessen(q, acc)

        def fill(d, X, halo0, halo1):
            for pc, (c0, c1) in enumerate(class_pairs(d)):
                new0 = shifted(d, 1, get(corr, c0), halo0(pc), pc)
                new1 = shifted(d, -1, get(corr, c1), halo1(pc), pc)
                for at in tiles:
                    X[c0, :, cols(*at)] = new0[at].astype(BF16)
                    X[c1, :, cols(*at)] = new1[at].astype(BF16)

        for copy in copies[2]:
            copy.wait()
        fill(2, Xz, lambda pc: read_y(fz, t, 0), lambda pc: read_y(fz, t, 1))
        if v == 0:
            for c0, c1 in class_pairs(2):
                S2[sb, c0] += corr[c1].astype(F32)
                S2[sb, c1] += Xz[c0].astype(F32)
        for copy in copies[1]:
            copy.wait()
        fill(1, Xy, lambda pc: read_y(fy, t, 0, pc), lambda pc: read_y(fy, t, 1, pc))
        for q in range(4):
            acc = dot(w_ref[2], pair(Xz, q))
            acc += dot(w_ref[6 if q % 2 == 0 else 5], pair(Xy, q ^ 1))
            lessen(q, acc)
        for copy in copies[0] + extra:
            copy.wait()
        fill(0, Xx, lambda pc: read_x(t, 0, pc), lambda pc: read_x(t, 1, pc))
        for q in range(4):
            lessen(q, dot(w_ref[4 if q // 2 == 0 else 3], pair(Xx, q ^ 2)))

    def class_order():
        r = lax.broadcasted_iota(jnp.int32, (D, 8 * Q), 0)
        k = lax.broadcasted_iota(jnp.int32, (D, 8 * Q), 1)
        for c in range(8):
            pick = jnp.where((k == r * 8 + c) & (r < Q), 1.0, 0.0).astype(BF16)
            p_rows[c * D:(c + 1) * D, :] = dot(pick, inverse_ref[...]).astype(BF16)
        k = lax.broadcasted_iota(jnp.int32, (8 * Q, 8 * D), 0)
        r = lax.broadcasted_iota(jnp.int32, (8 * Q, 8 * D), 1)
        q = r % D
        pick = jnp.where((k == q * 8 + r // D) & (q < Q), 1.0, 0.0).astype(BF16)
        p_ref[...] = dot(p_rows[...], pick).astype(BF16)

    def body(u, carry):
        @pl.when(u == 0)
        def _():
            move_x(True, 0, class_order)

        @pl.when(u == 2)
        def _():
            move_x(False, 1)
            for c in range(8):
                Sx[c] = S2[1, c]
            mxs_s[...] = S2[1, :4, :, :half].astype(BF16)
            sol_x().start()
            S2[1] = jnp.zeros_like(Sx)

        @pl.when(lax.rem(u, 2) == 0)
        def _():
            S2[0] = jnp.zeros_like(Sx)
            move_y(True, u)

        @pl.when(lax.rem(u, 2) == 1)
        def _():
            move_y(False, u)
            mys_s[...] = pack_y(S2.at[0], False).astype(BF16)
            sol_y(u).start()

        for v in (0, 1):
            t = 2 * u + v
            move_z(v == 0, t)
            colour(t, v, lax.rem(u, 2))

        @pl.when(lax.rem(u, 2) == 1)
        def _():
            sol_y(u).wait()
            for pc, (c0, c1) in enumerate(class_pairs(1)):
                S2[1, c0] += S2[0, c1]
                new = shifted(1, 1, get(S2.at[0], c0), read_y(mys, lax.div(u, 2), pc), pc)
                for at in tiles:
                    S2[1, c1, :, cols(*at)] += new[at]
        return carry

    lax.fori_loop(0, 4, body, 0)
    sol_x().wait()
    for pc, (c0, c1) in enumerate(class_pairs(0)):
        S2[1, c0] += Sx[c1]
        new = shifted(0, 1, get(Sx, c0), read_y(mxs, pc), pc)
        for at in tiles:
            S2[1, c1, :, cols(*at)] += new[at]

    for ref, out in ((S2.at[1], sol_ref), (R, res_ref)):
        for c in range(0, 8, 2):
            ox, oy = c // 4, c // 2 % 2
            for i, jh in tiles:
                x0 = ref[c, :, cols(i, jh)]
                x1 = ref[c + 1, :, cols(i, jh)]
                out[2 * i + ox, 4 * jh + oy] = jnp.where(jlo0, x0, roll(x1, nr))
                out[2 * i + ox, 4 * jh + 2 + oy] = jnp.where(jlo0, roll(x0, -nr), x1)


def in_blocks(sizes, right_side, cell_coef, cell_matrix, face_coupling, patch_inverse):
    Q = cell_matrix.shape[0]
    X, Y, Z = cell_coef.shape
    lanes = right_side.shape[3]
    nr = lanes // Z
    D = -(-(Q + 2) // 16) * 16
    ni, njh = X // 2, Y // 4
    assert lanes == LANES and ni == 2 and 4 * ni * njh * 2 * nr == LANES
    C = ni * njh * LANES
    coef = jnp.repeat(cell_coef, nr, axis=2)
    extra = jnp.stack([lax.rsqrt(coef), coef], 2)
    start = jnp.concatenate(
        [jnp.transpose(right_side, (1, 2, 0, 3)), extra, jnp.zeros((X, Y, D - Q - 2, lanes), F32)], 2)
    def padded(m):
        return jnp.pad(m, ((0, D - Q), (0, D - Q)))

    zero = jnp.zeros((D, D), F32)

    def both(a, b, c, d):
        return jnp.concatenate([jnp.concatenate([a, b], 1), jnp.concatenate([c, d], 1)], 0)

    m = padded(cell_matrix)
    f = [-padded(face_coupling[d]) for d in range(3)]
    ft = [x.T for x in f]
    mats = jnp.stack([
        both(m, zero, zero, m),
        both(zero, f[2], ft[2], zero),
        both(zero, ft[2], f[2], zero),
        both(f[0], zero, zero, f[0]),
        both(ft[0], zero, zero, ft[0]),
        both(f[1], zero, zero, f[1]),
        both(ft[1], zero, zero, ft[1]),
    ]).astype(BF16)
    half = njh * LANES
    V = pltpu.VMEM
    A = Q // 16 * 16
    assert Q == A + 1
    whole = (8, D, C)
    scratch = [
        V(whole, F32), V((2, *whole), F32), V(whole, F32), V(whole, BF16), V(whole, BF16), V(whole, BF16),
        V(whole, BF16), V(whole, BF16), V(whole, BF16),
        V((8, 2, 4, A, half), BF16), V((8, 2, 16, half), BF16),
        V((8, 2, 4, D, LANES), BF16), V((8, 2, D, LANES), BF16),
        V((2, 16, half), BF16), V((2, 4, D, LANES), BF16), V((2, D, LANES), BF16),
        V((2, 4, A, half), BF16), V((2, 4, 8, half), F32), V((4, D, half), BF16),
        V((4, 4, D, LANES), F32), V((2, 4, D, LANES), BF16), V((8, D, LANES), F32),
        V((4, A, half), BF16), V((4, D, half), BF16),
        V((4, D, LANES), F32), V((4, D, LANES), BF16), V((D, LANES), F32),
        V((8 * D, 8 * Q), BF16), V((8 * D, 8 * D), BF16),
        pltpu.SemaphoreType.DMA((96,)), pltpu.SemaphoreType.DMA((96,)),
    ]
    vmem = pl.BlockSpec(memory_space=pltpu.VMEM)
    sol, res = pl.pallas_call(
        functools.partial(block_kernel, sizes, (D, Q, nr, ni, njh)),
        out_shape=[jax.ShapeDtypeStruct((X, Y, D, lanes), F32)] * 2,
        in_specs=[vmem] * 3,
        out_specs=[vmem] * 2,
        scratch_shapes=scratch,
        compiler_params=pltpu.CompilerParams(
            collective_id=0, has_side_effects=True, vmem_limit_bytes=60 * 1024 * 1024),
    )(start, patch_inverse, mats)
    return tuple(jnp.transpose(x[:, :, :Q], (2, 0, 1, 3)) for x in (sol, res))


def fits_slabs(sizes, Q, X, Y, Z, lanes):
    group = sizes[0] * sizes[1]
    layers = Z // group
    return (lanes == LANES and Q % 16 == 1 and layers == 4 and Z == layers * group
            and (X // 2) * (Y // 2) == group and lanes // Z == 4 and 2 * layers == group
            and X % 2 == 0 and Y % 2 == 0)


def slab_kernel(sizes, dims, start_ref, coef_ref, inverse_ref, m_ref, f_ref, sol_ref, res_ref,
                msg, rx, R, S, X, B, W, P, XP, XM, YP, YM, U, p_rows,
                cr, rr, cr2, rsb, osol, ores, rsol, rres, send_sem, recv_sem):
    Q, nx, ny, nz, hx, hy = dims
    G = nx * ny
    L = 4
    A = Q - 1
    T = 4 * A
    D = T + 16
    wide = 1
    while wide * wide < nx:
        wide += 1
    lane = lax.broadcasted_iota(jnp.int32, (1, LANES), 1)
    row16 = lax.broadcasted_iota(jnp.int32, (16, LANES), 0)

    gx, gy, gz = [lax.axis_index(a) for a in AXES]
    mine = gx * ny + gy

    def snake(p):
        row = p // wide
        col = p % wide
        return row * wide + col + (row % 2) * (wide - 1 - 2 * col)

    def flip(p, plane):
        return p + (plane % 2) * (nx - 1 - 2 * p)

    slab = flip(snake(gx), gz) * ny + gy

    def device(plane, s):
        return {"gx": snake(flip(s // ny, plane)), "gy": s % ny, "gz": plane}

    def ring(step):
        g = lax.rem(gz * G + slab + step + nz * G, nz * G)
        return device(g // G, g % G)

    def in_plane(o):
        s = lax.rem(slab + o, G)
        return s, device(gz, s)

    barrier = pltpu.get_barrier_semaphore()
    for o in range(1, G):
        pl.semaphore_signal(barrier, inc=1, device_id=in_plane(o)[1], device_id_type=MESH)
    for step in (1, -1):
        pl.semaphore_signal(barrier, inc=1, device_id=ring(step), device_id_type=MESH)

    def remote(src, dst, k, where):
        return pltpu.make_async_remote_copy(
            src_ref=src, dst_ref=dst, send_sem=send_sem.at[k], recv_sem=recv_sem.at[k],
            device_id=where, device_id_type=MESH)

    def roll(x, s):
        s = s % LANES
        return pltpu.roll(x, s, 1) if s else x

    def swap(v, index_bit, weight):
        out = list(v)
        low = (lane // weight) % 2 == 0
        for n in range(len(v)):
            if n & index_bit:
                continue
            a, b = v[n], v[n | index_bit]
            out[n] = jnp.where(low, a, roll(b, weight))
            out[n | index_bit] = jnp.where(low, roll(a, -weight), b)
        return out

    bits = [1 << b for b in range(G.bit_length() - 1)]
    WS = 4 * L

    def swap_slab(v):
        for b in bits:
            v = swap(v, b, WS * b)
        return v

    def swap_source(v):
        for b in bits:
            v = swap(v, b, 2 * b)
        return v

    def lane_x(l):
        return (l // (2 * ny)) % nx * hx + (l // (WS * hy)) % hx

    def lane_y(l):
        return (l // 2) % ny * hy + (l // WS) % hy

    def shift_x(v, step):
        assert hx == 2
        i0 = (lane // (WS * hy)) % 2
        g = (lane // (2 * ny)) % nx
        half, one, all_ = WS * hy, 2 * ny, 2 * ny * (nx - 1)
        flat = roll(v, half)
        if step == 1:
            carry = jnp.where(g < nx - 1, roll(v, half - one), roll(v, half + all_))
            return jnp.where(i0 == 0, flat, carry)
        carry = jnp.where(g > 0, roll(v, half + one), roll(v, half - all_))
        return jnp.where(i0 == 1, flat, carry)

    def shift_y(v, step):
        assert ny == 2
        j0 = (lane // WS) % hy
        g = (lane // 2) % 2
        back = WS * (hy - 1)
        if step == 1:
            carry = jnp.where(g == 0, roll(v, back - 2), roll(v, back + 2))
            return jnp.where(j0 < hy - 1, roll(v, -WS), carry)
        carry = jnp.where(g == 0, roll(v, -back - 2), roll(v, -back + 2))
        return jnp.where(j0 > 0, roll(v, WS), carry)

    def class_rows(q):
        return slice(q * A, (q + 1) * A)

    cells = [(i, j) for i in range(hx) for j in range(hy)]

    def tail_tile(i, j):
        out = jnp.zeros((16, LANES), F32)
        for q in range(4):
            x, y = 2 * i + q // 2, 2 * j + q % 2
            k = coef_ref[x, y:y + 1, :]
            high = k.astype(BF16).astype(F32)
            out = jnp.where(row16 == q, start_ref[x, y, A:A + 1, :], out)
            out = jnp.where(row16 == 4 + q, high, out)
            out = jnp.where(row16 == 8 + q, k - high, out)
        return out

    for q in range(4):
        for r in range(0, A, 16):
            v = swap_slab([start_ref[2 * i + q // 2, 2 * j + q % 2, r:r + 16, :] for i, j in cells])
            for s in range(G):
                msg[s, q * A + r:q * A + r + 16, :] = v[s].astype(BF16)
    v = swap_slab([tail_tile(i, j) for i, j in cells])
    for s in range(G):
        msg[s, T:, :] = v[s].astype(BF16)
    pl.semaphore_wait(barrier, G + 1)
    arrivals = []
    for o in range(1, G):
        s, where = in_plane(o)
        arrivals.append(remote(msg.at[s], rx.at[mine], 32 + o, where))
        arrivals[-1].start()
    rx[mine] = msg[slab]

    def dot(a, b):
        return jnp.dot(a, b, preferred_element_type=F32)

    def dot_t(a, b):
        return lax.dot_general(a, b, (((1,), (1,)), ((), ())), preferred_element_type=F32)

    def iota(shape, d):
        return lax.broadcasted_iota(jnp.int32, shape, d)

    src, dst = iota((2 * LANES, 2 * LANES), 0), iota((2 * LANES, 2 * LANES), 1)
    same = (src // LANES == dst // LANES) & (src % 2 == dst % 2)
    sl, dl = src % LANES, dst % LANES
    for ref, step in ((XP, 1), (XM, hx * nx - 1)):
        hit = same & (lane_y(sl) == lane_y(dl)) & (lane_x(sl) == (lane_x(dl) + step) % (hx * nx))
        ref[...] = jnp.where(hit, 1.0, 0.0).astype(BF16)
    for ref, step in ((YP, 1), (YM, hy * ny - 1)):
        hit = same & (lane_x(sl) == lane_x(dl)) & (lane_y(sl) == (lane_y(dl) + step) % (hy * ny))
        ref[...] = jnp.where(hit, 1.0, 0.0).astype(BF16)

    def patch_row(k):
        d, c = k // 8, k % 8
        return c % 2 * D + jnp.where(d < A, c // 2 * A + d, T + c // 2)

    pick = patch_row(iota((2 * D, 8 * Q), 1)) == iota((2 * D, 8 * Q), 0)
    p_rows[...] = dot(jnp.where(pick, 1.0, 0.0).astype(BF16), inverse_ref[...]).astype(BF16)
    pick = patch_row(iota((8 * Q, 2 * D), 0)) == iota((8 * Q, 2 * D), 1)
    P[...] = dot(p_rows[...], jnp.where(pick, 1.0, 0.0).astype(BF16)).astype(BF16)

    def packed(k, n):
        q, d = k // n, k % n
        return jnp.where(d < A, q * A + d, jnp.where(d == A, T + q, -1))

    def one_hot(hit):
        return jnp.where(hit, 1.0, 0.0).astype(BF16)

    NR, NC = U.shape[0] // 4, U.shape[1] // 4
    rows_r = one_hot(packed(iota((D, 4 * NR), 1), NR) == iota((D, 4 * NR), 0))
    rows_c = one_hot(packed(iota((D, 4 * NC), 1), NC) == iota((D, 4 * NC), 0))
    cols_r = one_hot(packed(iota((4 * NR, D), 0), NR) == iota((4 * NR, D), 1))
    cols_c = one_hot(packed(iota((4 * NC, D), 0), NC) == iota((4 * NC, D), 1))

    def table(blocks):
        U[...] = jnp.zeros_like(U)
        for a, b, m in blocks:
            U[a * NR:a * NR + Q, b * NC:b * NC + Q] = m.astype(BF16)

    def plain():
        return dot(dot(rows_r, U[...]).astype(BF16), cols_c)

    def turned():
        return dot(dot_t(rows_c, U[...]).astype(BF16), cols_r)

    fx, fy, fz = f_ref[0], f_ref[1], f_ref[2]
    table([(q, q, -m_ref[...]) for q in range(4)])
    w = plain().astype(BF16)
    W[0, :, :D] = w
    W[1, :, :D] = w
    table([(0, 2, fx), (1, 3, fx), (0, 1, fy), (2, 3, fy)])
    w = (plain() + turned()).astype(BF16)
    W[0, :, D:2 * D] = w
    W[1, :, D:2 * D] = w
    table([(2, 0, fx), (3, 1, fx)])
    w = (plain() + turned()).astype(BF16)
    W[0, :, 2 * D:3 * D] = w
    W[1, :, 2 * D:3 * D] = w
    table([(1, 0, fy), (3, 2, fy)])
    w = (plain() + turned()).astype(BF16)
    W[0, :, 3 * D:4 * D] = w
    W[1, :, 3 * D:4 * D] = w
    table([(q, q, fz) for q in range(4)])
    W[0, :, 4 * D:] = plain().astype(BF16)
    W[1, :, 4 * D:] = turned().astype(BF16)
    S[...] = jnp.zeros_like(S)

    def z_up(c):
        return dot(W[0, :, 4 * D:], c)

    def z_down(c):
        return dot(W[1, :, 4 * D:], c)

    for copy in arrivals:
        copy.wait()
    for r in range(0, D, 16):
        v = swap_source([rx[n, r:r + 16, :].astype(F32) for n in range(G)])
        for n in range(G):
            z, h = n // 2, n % 2
            R[h, z + 1 - h, r:r + 16, :] = v[n]

    def move(ref, h, idx, d, down):
        shift = shift_x if d == 0 else shift_y
        bit = 2 >> d
        for q in range(4):
            if q & bit:
                continue
            old0 = ref[h, idx, class_rows(q), :]
            old1 = ref[h, idx, class_rows(q + bit), :]
            if down:
                ref[h, idx, class_rows(q), :] = shift(old1, -1)
                ref[h, idx, class_rows(q + bit), :] = old0
            else:
                ref[h, idx, class_rows(q), :] = old1
                ref[h, idx, class_rows(q + bit), :] = shift(old0, 1)
        t = ref[h, idx, T:, :]
        upper = (row16 // bit) % 2 == 1
        if down:
            t = jnp.where(upper, shift(t, -1), t)
        else:
            t = jnp.where(upper, t, shift(t, 1))
        ref[h, idx, T:, :] = jnp.where(upper, pltpu.roll(t, bit, 0), pltpu.roll(t, 16 - bit, 0))

    copies = []
    for h in (0, 1):
        for z in range(L):
            for d in (0, 1):
                move(R, h, z + 1 - h, d, True)
        end, step = (L, 1) if h == 0 else (0, -1)
        rsb[h] = R[h, end].astype(BF16)
        copies.append(remote(rsb.at[h], cr2.at[h], 40 + h, ring(step)))
        copies[-1].start()
    for h in (0, 1):
        copies[h].wait()
        R[h, 0 if h == 0 else L] = cr2[h].astype(F32)
        for idx in range(L + 1):
            t = R[h, idx, T:, :]
            k = t + pltpu.roll(t, 12, 0)
            k = jnp.where((row16 >= 4) & (row16 < 8), k, 1.0)
            s = pltpu.roll(lax.rsqrt(k), 4, 0)
            t = jnp.where(row16 < 4, t, jnp.where(row16 < 8, k, jnp.where(row16 < 12, s, 0.0)))
            R[h, idx, T:, :] = t

    def split(k):
        return k % 2, slice(k // 2 * LANES, (k // 2 + 1) * LANES)

    def c_copy(h, base, t, low):
        z, part = split(0 if low else L - 1)
        return remote(B.at[h, z, D:2 * D, part], cr.at[t, h], t * 4 + h, ring(-1 if low else 1))

    def r_copy(h, base, t, low):
        return remote(rsb.at[h], rr.at[t, h], t * 4 + 2 + h, ring(-1 if low else 1))

    def c2_copy(h, low):
        z, part = split(0 if low else L - 1)
        return remote(B.at[h, z, D:2 * D, part], cr2.at[h], 42 + h, ring(-1 if low else 1))

    def begin(h, base, t, even, last):
        low = base == 0
        first = 0 if low else 1
        for k in range(L):
            z, part = split(k)
            for q in range(4):
                s = R[h, base + k, T + 8 + q:T + 9 + q, :]
                X[h, z * D + q * A:z * D + (q + 1) * A, part] = (
                    R[h, base + k, class_rows(q), :] * s).astype(BF16)
            t16 = R[h, base + k, T:, :]
            x16 = jnp.where(row16 < 4, t16 * pltpu.roll(t16, 8, 0), 0.0)
            X[h, z * D + T:(z + 1) * D, part] = x16.astype(BF16)

        def solve(z):
            got = dot(P[z * D:(z + 1) * D, :], X[h])
            for p in (0, 1):
                idx = base + 2 * p + z
                part = slice(p * LANES, (p + 1) * LANES)
                end = 2 * p + z == (0 if low else L - 1)
                t16 = R[h, idx, T:, :]
                for q in range(5):
                    if q < 4:
                        at = class_rows(q)
                        s = t16[8 + q:9 + q]
                        k = t16[4 + q:5 + q]
                    else:
                        at = slice(T, D)
                        s = jnp.where(row16 < 4, pltpu.roll(t16, 8, 0), 0.0)
                        k = jnp.where(row16 < 4, pltpu.roll(t16, 12, 0), 0.0)
                    c = got[at, part] * s
                    if not (even and end):
                        S[h, idx, at, :] += c
                    cb = c.astype(BF16)
                    B[h, z, at, part] = (c * k).astype(BF16)
                    B[h, z, D + at.start:D + at.stop, part] = cb
                    B[h, 1 - z, 4 * D + at.start:4 * D + at.stop, part] = cb

        def neighbours(z):
            c = B[h, z, D:2 * D, :]
            t = c[T:]
            r16 = lax.broadcasted_iota(jnp.int32, (16, 2 * LANES), 0)
            xp = dot(jnp.concatenate([c[:2 * A], t], 0), XP[...])
            xm = dot(jnp.concatenate([c[2 * A:T], t], 0), XM[...])
            yp = dot(jnp.concatenate([c[:A], c[2 * A:3 * A], t], 0), YP[...])
            ym = dot(jnp.concatenate([c[A:2 * A], c[3 * A:T], t], 0), YM[...])
            o = 2 * D
            B[h, z, o:o + 2 * A, :] = xp[:2 * A].astype(BF16)
            B[h, z, o + 2 * A:o + T, :] = xm[:2 * A].astype(BF16)
            B[h, z, o + T:o + D, :] = jnp.where(r16 < 2, xp[2 * A:], xm[2 * A:]).astype(BF16)
            o = 3 * D
            B[h, z, o:o + A, :] = yp[:A].astype(BF16)
            B[h, z, o + A:o + 2 * A, :] = ym[:A].astype(BF16)
            B[h, z, o + 2 * A:o + 3 * A, :] = yp[A:2 * A].astype(BF16)
            B[h, z, o + 3 * A:o + T, :] = ym[A:2 * A].astype(BF16)
            B[h, z, o + T:o + D, :] = jnp.where(r16 % 2 == 0, yp[2 * A:], ym[2 * A:]).astype(BF16)

        def apply(z):
            acc = dot(W[z], B[h, z])
            for p in (0, 1):
                R[h, base + 2 * p + z] += acc[:, p * LANES:(p + 1) * LANES]

        solve(first)
        c_copy(h, base, t, low).start()
        solve(1 - first)
        if last is not None:
            @pl.when(last)
            def _():
                c2_copy(h, not low).start()
        neighbours(first)
        apply(first)
        end = base if low else base + L - 1

        def send_r():
            rsb[h] = R[h, end].astype(BF16)
            r_copy(h, base, t, low).start()

        if last is None:
            send_r()
        else:
            pl.when(jnp.logical_not(last))(send_r)
        neighbours(1 - first)
        apply(1 - first)
        if low:
            acc = z_down(B[h, 1, D:2 * D, :])
            R[h, base + 2] += acc[:, :LANES]
            new, out = acc[:, LANES:], base + L
            R[h, base + 1] += z_up(B[h, 0, D:2 * D, LANES:])
        else:
            acc = z_up(B[h, 0, D:2 * D, :])
            R[h, base + 1] += acc[:, LANES:]
            new, out = acc[:, :LANES], base - 1
            R[h, base + 2] += z_down(B[h, 1, D:2 * D, :LANES])
        R[h, out, :T, :] = new[:T]
        R[h, out, T:T + 4, :] = new[T:T + 4]

    def finish(h, base, t, even, last):
        low = base == 0
        near, out = (base + L - 1, base + L) if low else (base, base - 1)
        c_copy(h, base, t, low).wait()
        c = cr[t, h]
        R[h, near] += z_up(c) if low else z_down(c)
        if even:
            S[h, out] += c.astype(F32)

        def take():
            r_copy(h, base, t, low).wait()
            R[h, out, :T, :] += rr[t, h, :T, :].astype(F32)
            R[h, out, T:T + 4, :] += rr[t, h, T:, :].astype(F32)[:4]

        if last is None:
            take()
        else:
            pl.when(jnp.logical_not(last))(take)

            @pl.when(last)
            def _():
                c2_copy(h, not low).wait()
                other = base if low else base + L - 1
                R[h, other] += z_down(cr2[h]) if low else z_up(cr2[h])

    def between(h, u):
        def shift(d, down):
            for idx in range(L + 1):
                move(R, h, idx, d, down)
            for z in range(L):
                move(S, h, z + 1 - h, d, down)

        @pl.when(lax.rem(u, 2) == 0)
        def _():
            shift(1, False)

        @pl.when(u == 1)
        def _():
            shift(0, False)
            shift(1, True)

    def body(u, carry):
        begin(0, 0, 2 * u, True, None)

        @pl.when(u > 0)
        def _():
            finish(1, 0, 2 * u - 1, False, None)
            between(1, u - 1)

        begin(1, 1, 2 * u, True, None)
        finish(0, 0, 2 * u, True, None)
        begin(0, 1, 2 * u + 1, False, u == 3)
        finish(1, 1, 2 * u, True, None)
        begin(1, 0, 2 * u + 1, False, u == 3)
        finish(0, 1, 2 * u + 1, False, u == 3)

        @pl.when(u < 3)
        def _():
            between(0, u)
        return carry

    lax.fori_loop(0, 4, body, 0)

    def cut(ref, out):
        for r in range(0, D, 16):
            v = swap_source([ref[n % 2, n // 2 + 1 - n % 2, r:r + 16, :] for n in range(G)])
            for n in range(G):
                out[n, r:r + 16, :] = v[n].astype(BF16)

    def ship(out, got, k):
        sent = []
        for o in range(1, G):
            s, where = in_plane(o)
            sent.append(remote(out.at[where["gx"] * ny + where["gy"]], got.at[slab], k + o, where))
            sent[-1].start()
        got[slab] = out[mine]
        return sent

    def unpack(got, out):
        for q in range(4):
            for r in range(0, A, 16):
                v = swap_slab([got[s, q * A + r:q * A + r + 16, :].astype(F32) for s in range(G)])
                for (i, j), x in zip(cells, v):
                    out[2 * i + q // 2, 2 * j + q % 2, r:r + 16, :] = x
        v = swap_slab([got[s, T:, :].astype(F32) for s in range(G)])
        for (i, j), x in zip(cells, v):
            for q in range(4):
                out[2 * i + q // 2, 2 * j + q % 2, A:A + 1, :] = x[q:q + 1]

    cut(S, osol)
    first = ship(osol, rsol, 48)
    finish(1, 0, 7, False, jnp.bool_(True))
    cut(R, ores)
    second = ship(ores, rres, 56)
    for copy in first:
        copy.wait()
    unpack(rsol, sol_ref)
    for copy in second:
        copy.wait()
    unpack(rres, res_ref)


def in_slabs(sizes, right_side, cell_coef, cell_matrix, face_coupling, patch_inverse):
    Q = cell_matrix.shape[0]
    X, Y, Z = cell_coef.shape
    lanes = right_side.shape[3]
    nx, ny, nz = sizes
    G = nx * ny
    D = 4 * (Q - 1) + 16
    start = jnp.transpose(right_side, (1, 2, 0, 3))
    coef = jnp.repeat(cell_coef, lanes // Z, axis=2)
    V = pltpu.VMEM
    half = (D, LANES)
    side = (2 * LANES, 2 * LANES)
    scratch = [
        V((G, *half), BF16), V((G, *half), BF16),
        V((2, 5, *half), F32), V((2, 5, *half), F32),
        V((2, 2 * D, 2 * LANES), BF16), V((2, 2, 5 * D, 2 * LANES), BF16),
        V((2, D, 5 * D), BF16), V((2 * D, 2 * D), BF16),
        V(side, BF16), V(side, BF16), V(side, BF16), V(side, BF16),
        V((4 * 96, 4 * LANES), BF16), V((2 * D, 8 * Q), BF16),
        V((8, 2, *half), BF16), V((8, 2, *half), BF16), V((2, *half), BF16), V((2, *half), BF16),
        V((G, *half), BF16), V((G, *half), BF16), V((G, *half), BF16), V((G, *half), BF16),
        pltpu.SemaphoreType.DMA((64,)), pltpu.SemaphoreType.DMA((64,)),
    ]
    vmem = pl.BlockSpec(memory_space=pltpu.VMEM)
    sol, res = pl.pallas_call(
        functools.partial(slab_kernel, sizes, (Q, nx, ny, nz, X // 2, Y // 2)),
        out_shape=[jax.ShapeDtypeStruct((X, Y, Q, lanes), F32)] * 2,
        in_specs=[vmem] * 5,
        out_specs=[vmem] * 2,
        scratch_shapes=scratch,
        compiler_params=pltpu.CompilerParams(
            collective_id=0, has_side_effects=True, vmem_limit_bytes=60 * 1024 * 1024),
    )(start, coef, patch_inverse, cell_matrix, face_coupling)
    return tuple(jnp.transpose(x, (2, 0, 1, 3)) for x in (sol, res))


def on_device(sizes, right_side, cell_coef, cell_matrix, face_coupling, patch_inverse):
    X, Y, Z = cell_coef.shape
    form = in_slabs if fits_slabs(sizes, cell_matrix.shape[0], X, Y, Z, right_side.shape[3]) else in_blocks
    return form(sizes, right_side, cell_coef, cell_matrix, face_coupling, patch_inverse)


def solution(mesh):
    sizes = tuple(mesh.shape[a] for a in AXES)
    placed = (P(None, "gx", "gy", "gz"), P("gx", "gy", "gz"), P(), P(), P())
    return jax.shard_map(
        functools.partial(on_device, sizes),
        mesh=mesh,
        in_specs=placed,
        out_specs=(P(None, "gx", "gy", "gz"), P(None, "gx", "gy", "gz")),
        check_vma=False,
    )
```

```python
import functools
import jax
import jax.numpy as jnp
from jax import lax
from jax.experimental import pallas as pl
from jax.experimental.pallas import tpu as pltpu
from jax.sharding import PartitionSpec as P

AXES = ("gx", "gy", "gz")
MESH = pl.DeviceIdType.MESH
F32, BF16 = jnp.float32, jnp.bfloat16
LANES = 128


def class_pairs(d):
    bit = 4 >> d
    return [(c, c + bit) for c in range(8) if not c & bit]


def block_kernel(sizes, dims, start_ref, inverse_ref, w_ref, sol_ref, res_ref,
           R, S2, Sx, scaled, corr, ccorr, Xx, Xy, Xz,
           fx, fxe, fy, fz, fxes, fys, fzs, mxr, mxe, mxs, myr, mys, mzr,
           mxr_s, mxs_s, myr_s, mys_s, mzr_s, p_rows, p_ref, send_sem, recv_sem):
    D, Q, nr, ni, njh = dims
    w = 2 * nr
    A = Q // 16 * 16
    tiles = [(i, jh) for i in range(ni) for jh in range(njh)]
    C = ni * njh * LANES
    half = njh * LANES
    lane = lax.broadcasted_iota(jnp.int32, (D, LANES), 1)
    jlo0 = (lane // nr) % 2 == 0
    piece = lane // w

    me = [lax.axis_index(a) for a in AXES]

    def neighbour(d, step):
        n = sizes[d]
        return {AXES[d]: lax.rem(me[d] + step + n, n)}

    barrier = pltpu.get_barrier_semaphore()
    for d in range(3):
        for step in (1, -1):
            pl.semaphore_signal(barrier, inc=1, device_id=neighbour(d, step), device_id_type=MESH)

    def rows(c):
        return slice(c * D, (c + 1) * D)

    def cols(i, jh):
        t = i * njh + jh
        return slice(t * LANES, (t + 1) * LANES)

    def get(ref, c):
        return {t: ref[c, :, cols(*t)].astype(F32) for t in tiles}

    def roll(x, s):
        s = s % LANES
        return pltpu.roll(x, s, 1) if s else x

    for c in range(0, 8, 2):
        ox, oy = c // 4, c // 2 % 2
        for i, jh in tiles:
            a = start_ref[2 * i + ox, 4 * jh + oy]
            b = start_ref[2 * i + ox, 4 * jh + 2 + oy]
            R[c, :, cols(i, jh)] = jnp.where(jlo0, a, roll(b, nr))
            R[c + 1, :, cols(i, jh)] = jnp.where(jlo0, roll(a, -nr), b)
    S2[...] = jnp.zeros_like(S2)
    pl.semaphore_wait(barrier, 6)

    def pack_y(ref, last):
        out = []
        for p in class_pairs(1):
            c = p[1] if last else p[0]
            jh = njh - 1 if last else 0
            t0 = ref[c, :, cols(0, jh)].astype(F32)
            t1 = ref[c, :, cols(1, jh)].astype(F32)
            if last:
                out.append(jnp.where(jlo0, roll(t1, -nr), t0))
            else:
                out.append(jnp.where(jlo0, t0, roll(t1, nr)))
        return jnp.stack(out, 0)

    def pack_z(ref, last):
        acc = jnp.zeros((D, LANES), F32)
        n = 0
        for p in class_pairs(2):
            c = p[1] if last else p[0]
            for t in tiles:
                x = ref[c, :, cols(*t)].astype(F32)
                x = roll(x, w * (n + 1) if last else w * n)
                acc = jnp.where(piece == n, x, acc)
                n += 1
        return acc

    def shifted(d, step, have, halo, pc):
        out = {}
        for i, jh in tiles:
            if d == 0:
                at = i + step
                if 0 <= at < ni:
                    new = have[at, jh]
                else:
                    new = halo(slice(jh * LANES, (jh + 1) * LANES))
            elif d == 1:
                at = jh + step
                if 0 <= at < njh:
                    other = roll(have[i, at], step * nr)
                else:
                    other = halo(slice(0, LANES))
                    if i == 0:
                        other = roll(other, step * nr)
                cur = roll(have[i, jh], -step * nr)
                new = jnp.where(jlo0, cur, other) if step == 1 else jnp.where(jlo0, other, cur)
            else:
                n = pc * len(tiles) + i * njh + jh
                h = halo(slice(0, LANES))
                if step == 1:
                    new = jnp.where(lane >= LANES - w, roll(h, LANES - w - w * n),
                                    roll(have[i, jh], -w))
                else:
                    new = jnp.where(lane < w, roll(h, -w * n), roll(have[i, jh], w))
            out[i, jh] = new
        return out

    def read_x(t, last, pc):
        first = lax.broadcasted_iota(jnp.int32, (D - A, LANES), 0) == 0

        def halo(c):
            tail = fxe[t, last, :, c].astype(F32)[pc:pc + 1]
            return jnp.concatenate(
                [fx[t, last, pc, :, c].astype(F32), jnp.where(first, tail, 0.0)], 0)
        return halo

    def read_y(ref, *at):
        return lambda c: ref[(*at, slice(None), c)].astype(F32)

    def remote(src, dst, k, d, step):
        return pltpu.make_async_remote_copy(
            src_ref=src, dst_ref=dst, send_sem=send_sem.at[k], recv_sem=recv_sem.at[k],
            device_id=neighbour(d, step), device_id_type=MESH)

    def move(d, down, copies, halo, beside=None):
        for copy in copies:
            copy.start()
        if beside is not None:
            beside()
        for copy in copies:
            copy.wait()
        for pc, (c0, c1) in enumerate(class_pairs(d)):
            old0, old1 = get(R, c0), get(R, c1)
            if down:
                new0, new1 = shifted(d, -1, old1, halo(pc), pc), old0
            else:
                new0, new1 = old1, shifted(d, 1, old0, halo(pc), pc)
            for t in tiles:
                R[c0, :, cols(*t)] = new0[t]
                R[c1, :, cols(*t)] = new1[t]

    def move_x(down, at, beside=None):
        part = slice((ni - 1) * half, ni * half) if down else slice(0, half)
        cs = slice(4, 8) if down else slice(0, 4)
        mxr_s[...] = R[cs, :A, part].astype(BF16)
        step = 1 if down else -1
        copies = [remote(mxr_s, mxr.at[at], 72 + at, 0, step),
                  remote(R.at[cs, A:A + 8, part], mxe.at[at], 74 + at, 0, step)]
        zeros = jnp.zeros((D - A - 8, LANES), F32)

        def halo(pc):
            return lambda c: jnp.concatenate(
                [mxr[at, pc, :, c].astype(F32), mxe[at, pc, :, c], zeros], 0)
        move(0, down, copies, halo, beside)

    def move_y(down, u):
        myr_s[...] = pack_y(R, down)
        move(1, down, [remote(myr_s, myr.at[u], 64 + u, 1, 1 if down else -1)],
             lambda pc: read_y(myr, u, pc))

    def move_z(down, t):
        mzr_s[...] = pack_z(R, down)
        move(2, down, [remote(mzr_s, mzr.at[t], 48 + t, 2, 1 if down else -1)],
             lambda pc: read_y(mzr, t))

    def sol_y(u):
        return remote(mys_s, mys.at[lax.div(u, 2)], 56 + lax.div(u, 2), 1, -1)

    def sol_x():
        return remote(mxs_s, mxs, 58, 0, -1)

    def pair(ref, q):
        return ref[2 * q:2 * q + 2].reshape(2 * D, C)

    def lessen(q, acc):
        R[2 * q:2 * q + 2] -= acc.reshape(2, D, C)

    def dot(a, b):
        return jnp.dot(a, b, preferred_element_type=F32)

    def colour(t, v, sb):
        for c in range(8):
            s = R[c, Q:Q + 1, :]
            scaled[c] = (s * R[c]).astype(BF16)
        copies = [[None, None] for _ in range(3)]
        extra = [None, None]
        line = lax.broadcasted_iota(jnp.int32, (16, half), 0)
        for n in range(ni):
            part = slice(n * half, (n + 1) * half)
            solved = dot(p_ref[...], scaled[:, :, part].reshape(8 * D, half))
            for c in range(8):
                s = R[c, Q:Q + 1, part]
                k = R[c, Q + 1:Q + 2, part]
                got = s * solved[rows(c), :]
                if v == 1:
                    S2[sb, c, :, part] += got
                corr[c, :, part] = got.astype(BF16)
                ccorr[c, :, part] = (k * got).astype(BF16)
            for last in (0, 1):
                if n != (ni - 1 if last else 0):
                    continue
                step = 1 if last else -1
                tail = jnp.zeros((16, half), F32)
                for pc in range(4):
                    row = corr[4 * last + pc, A:, part].astype(F32)[:1]
                    tail = jnp.where(line == pc, row, tail)
                fxes[last] = tail.astype(BF16)
                copies[0][last] = remote(corr.at[4 * last:4 * last + 4, :A, part], fx.at[t, last],
                                         t * 6 + last, 0, step)
                copies[0][last].start()
                extra[last] = remote(fxes.at[last], fxe.at[t, last], 80 + 2 * t + last, 0, step)
                extra[last].start()
        for last in (0, 1):
            fzs[last] = pack_z(corr, last).astype(BF16)
            copies[2][last] = remote(fzs.at[last], fz.at[t, last], t * 6 + 4 + last, 2, 1 if last else -1)
            copies[2][last].start()
        for last in (0, 1):
            fys[last] = pack_y(corr, last).astype(BF16)
            copies[1][last] = remote(fys.at[last], fy.at[t, last], t * 6 + 2 + last, 1, 1 if last else -1)
            copies[1][last].start()
        for q in range(4):
            acc = dot(w_ref[0], pair(ccorr, q))
            acc += dot(w_ref[1], pair(corr, q))
            acc += dot(w_ref[3 if q // 2 == 0 else 4], pair(corr, q ^ 2))
            acc += dot(w_ref[5 if q % 2 == 0 else 6], pair(corr, q ^ 1))
            lessen(q, acc)

        def fill(d, X, halo0, halo1):
            for pc, (c0, c1) in enumerate(class_pairs(d)):
                new0 = shifted(d, 1, get(corr, c0), halo0(pc), pc)
                new1 = shifted(d, -1, get(corr, c1), halo1(pc), pc)
                for at in tiles:
                    X[c0, :, cols(*at)] = new0[at].astype(BF16)
                    X[c1, :, cols(*at)] = new1[at].astype(BF16)

        for copy in copies[2]:
            copy.wait()
        fill(2, Xz, lambda pc: read_y(fz, t, 0), lambda pc: read_y(fz, t, 1))
        if v == 0:
            for c0, c1 in class_pairs(2):
                S2[sb, c0] += corr[c1].astype(F32)
                S2[sb, c1] += Xz[c0].astype(F32)
        for copy in copies[1]:
            copy.wait()
        fill(1, Xy, lambda pc: read_y(fy, t, 0, pc), lambda pc: read_y(fy, t, 1, pc))
        for q in range(4):
            acc = dot(w_ref[2], pair(Xz, q))
            acc += dot(w_ref[6 if q % 2 == 0 else 5], pair(Xy, q ^ 1))
            lessen(q, acc)
        for copy in copies[0] + extra:
            copy.wait()
        fill(0, Xx, lambda pc: read_x(t, 0, pc), lambda pc: read_x(t, 1, pc))
        for q in range(4):
            lessen(q, dot(w_ref[4 if q // 2 == 0 else 3], pair(Xx, q ^ 2)))

    def class_order():
        r = lax.broadcasted_iota(jnp.int32, (D, 8 * Q), 0)
        k = lax.broadcasted_iota(jnp.int32, (D, 8 * Q), 1)
        for c in range(8):
            pick = jnp.where((k == r * 8 + c) & (r < Q), 1.0, 0.0).astype(BF16)
            p_rows[c * D:(c + 1) * D, :] = dot(pick, inverse_ref[...]).astype(BF16)
        k = lax.broadcasted_iota(jnp.int32, (8 * Q, 8 * D), 0)
        r = lax.broadcasted_iota(jnp.int32, (8 * Q, 8 * D), 1)
        q = r % D
        pick = jnp.where((k == q * 8 + r // D) & (q < Q), 1.0, 0.0).astype(BF16)
        p_ref[...] = dot(p_rows[...], pick).astype(BF16)

    def body(u, carry):
        @pl.when(u == 0)
        def _():
            move_x(True, 0, class_order)

        @pl.when(u == 2)
        def _():
            move_x(False, 1)
            for c in range(8):
                Sx[c] = S2[1, c]
            mxs_s[...] = S2[1, :4, :, :half].astype(BF16)
            sol_x().start()
            S2[1] = jnp.zeros_like(Sx)

        @pl.when(lax.rem(u, 2) == 0)
        def _():
            S2[0] = jnp.zeros_like(Sx)
            move_y(True, u)

        @pl.when(lax.rem(u, 2) == 1)
        def _():
            move_y(False, u)
            mys_s[...] = pack_y(S2.at[0], False).astype(BF16)
            sol_y(u).start()

        for v in (0, 1):
            t = 2 * u + v
            move_z(v == 0, t)
            colour(t, v, lax.rem(u, 2))

        @pl.when(lax.rem(u, 2) == 1)
        def _():
            sol_y(u).wait()
            for pc, (c0, c1) in enumerate(class_pairs(1)):
                S2[1, c0] += S2[0, c1]
                new = shifted(1, 1, get(S2.at[0], c0), read_y(mys, lax.div(u, 2), pc), pc)
                for at in tiles:
                    S2[1, c1, :, cols(*at)] += new[at]
        return carry

    lax.fori_loop(0, 4, body, 0)
    sol_x().wait()
    for pc, (c0, c1) in enumerate(class_pairs(0)):
        S2[1, c0] += Sx[c1]
        new = shifted(0, 1, get(Sx, c0), read_y(mxs, pc), pc)
        for at in tiles:
            S2[1, c1, :, cols(*at)] += new[at]

    for ref, out in ((S2.at[1], sol_ref), (R, res_ref)):
        for c in range(0, 8, 2):
            ox, oy = c // 4, c // 2 % 2
            for i, jh in tiles:
                x0 = ref[c, :, cols(i, jh)]
                x1 = ref[c + 1, :, cols(i, jh)]
                out[2 * i + ox, 4 * jh + oy] = jnp.where(jlo0, x0, roll(x1, nr))
                out[2 * i + ox, 4 * jh + 2 + oy] = jnp.where(jlo0, roll(x0, -nr), x1)


def in_blocks(sizes, right_side, cell_coef, cell_matrix, face_coupling, patch_inverse):
    Q = cell_matrix.shape[0]
    X, Y, Z = cell_coef.shape
    lanes = right_side.shape[3]
    nr = lanes // Z
    D = -(-(Q + 2) // 16) * 16
    ni, njh = X // 2, Y // 4
    assert lanes == LANES and ni == 2 and 4 * ni * njh * 2 * nr == LANES
    C = ni * njh * LANES
    coef = jnp.repeat(cell_coef, nr, axis=2)
    extra = jnp.stack([lax.rsqrt(coef), coef], 2)
    start = jnp.concatenate(
        [jnp.transpose(right_side, (1, 2, 0, 3)), extra, jnp.zeros((X, Y, D - Q - 2, lanes), F32)], 2)
    def padded(m):
        return jnp.pad(m, ((0, D - Q), (0, D - Q)))

    zero = jnp.zeros((D, D), F32)

    def both(a, b, c, d):
        return jnp.concatenate([jnp.concatenate([a, b], 1), jnp.concatenate([c, d], 1)], 0)

    m = padded(cell_matrix)
    f = [-padded(face_coupling[d]) for d in range(3)]
    ft = [x.T for x in f]
    mats = jnp.stack([
        both(m, zero, zero, m),
        both(zero, f[2], ft[2], zero),
        both(zero, ft[2], f[2], zero),
        both(f[0], zero, zero, f[0]),
        both(ft[0], zero, zero, ft[0]),
        both(f[1], zero, zero, f[1]),
        both(ft[1], zero, zero, ft[1]),
    ]).astype(BF16)
    half = njh * LANES
    V = pltpu.VMEM
    A = Q // 16 * 16
    assert Q == A + 1
    whole = (8, D, C)
    scratch = [
        V(whole, F32), V((2, *whole), F32), V(whole, F32), V(whole, BF16), V(whole, BF16), V(whole, BF16),
        V(whole, BF16), V(whole, BF16), V(whole, BF16),
        V((8, 2, 4, A, half), BF16), V((8, 2, 16, half), BF16),
        V((8, 2, 4, D, LANES), BF16), V((8, 2, D, LANES), BF16),
        V((2, 16, half), BF16), V((2, 4, D, LANES), BF16), V((2, D, LANES), BF16),
        V((2, 4, A, half), BF16), V((2, 4, 8, half), F32), V((4, D, half), BF16),
        V((4, 4, D, LANES), F32), V((2, 4, D, LANES), BF16), V((8, D, LANES), F32),
        V((4, A, half), BF16), V((4, D, half), BF16),
        V((4, D, LANES), F32), V((4, D, LANES), BF16), V((D, LANES), F32),
        V((8 * D, 8 * Q), BF16), V((8 * D, 8 * D), BF16),
        pltpu.SemaphoreType.DMA((96,)), pltpu.SemaphoreType.DMA((96,)),
    ]
    vmem = pl.BlockSpec(memory_space=pltpu.VMEM)
    sol, res = pl.pallas_call(
        functools.partial(block_kernel, sizes, (D, Q, nr, ni, njh)),
        out_shape=[jax.ShapeDtypeStruct((X, Y, D, lanes), F32)] * 2,
        in_specs=[vmem] * 3,
        out_specs=[vmem] * 2,
        scratch_shapes=scratch,
        compiler_params=pltpu.CompilerParams(
            collective_id=0, has_side_effects=True, vmem_limit_bytes=60 * 1024 * 1024),
    )(start, patch_inverse, mats)
    return tuple(jnp.transpose(x[:, :, :Q], (2, 0, 1, 3)) for x in (sol, res))


def fits_slabs(sizes, Q, X, Y, Z, lanes):
    group = sizes[0] * sizes[1]
    layers = Z // group
    return (lanes == LANES and Q % 16 == 1 and layers == 4 and Z == layers * group
            and (X // 2) * (Y // 2) == group and lanes // Z == 4 and 2 * layers == group
            and X % 2 == 0 and Y % 2 == 0)


def slab_kernel(sizes, dims, right_ref, coef_ref, inverse_ref, m_ref, f_ref, sol_out, res_out,
                start_ref, sol_ref, res_ref, coef_high, coef_low, msg, rx, R, S, X, B, W, P, XP, XM, YP, YM, U, p_rows,
                cr, rr, cr2, rsb, osol, ores, rsol, rres, send_sem, recv_sem, load_sem, store_sem):
    Q, nx, ny, nz, hx, hy = dims
    G = nx * ny
    L = 4
    A = Q - 1
    T = 4 * A
    D = T + 16
    wide = 1
    while wide * wide < nx:
        wide += 1
    lane = lax.broadcasted_iota(jnp.int32, (1, LANES), 1)
    row16 = lax.broadcasted_iota(jnp.int32, (16, LANES), 0)

    gx, gy, gz = [lax.axis_index(a) for a in AXES]
    mine = gx * ny + gy

    def snake(p):
        row = p // wide
        col = p % wide
        return row * wide + col + (row % 2) * (wide - 1 - 2 * col)

    def flip(p, plane):
        return p + (plane % 2) * (nx - 1 - 2 * p)

    slab = flip(snake(gx), gz) * ny + gy

    def device(plane, s):
        return {"gx": snake(flip(s // ny, plane)), "gy": s % ny, "gz": plane}

    def ring(step):
        g = lax.rem(gz * G + slab + step + nz * G, nz * G)
        return device(g // G, g % G)

    def in_plane(o):
        s = lax.rem(slab + o, G)
        return s, device(gz, s)

    places = [(x, y) for x in range(2 * hx) for y in range(2 * hy)]

    def local(src, dst, sem, k):
        return pltpu.make_async_copy(src, dst, sem.at[k])

    def load(k):
        x, y = places[k]
        return local(right_ref.at[:, x, y, :], start_ref.at[x, y], load_sem, k)

    def store(ref, out, k, first):
        x, y = places[k]
        return local(ref.at[x, y], out.at[:, x, y, :], store_sem, first + k)

    for k in range(len(places)):
        load(k).start()

    barrier = pltpu.get_barrier_semaphore()
    for o in range(1, G):
        pl.semaphore_signal(barrier, inc=1, device_id=in_plane(o)[1], device_id_type=MESH)
    for step in (1, -1):
        pl.semaphore_signal(barrier, inc=1, device_id=ring(step), device_id_type=MESH)

    def remote(src, dst, k, where):
        return pltpu.make_async_remote_copy(
            src_ref=src, dst_ref=dst, send_sem=send_sem.at[k], recv_sem=recv_sem.at[k],
            device_id=where, device_id_type=MESH)

    def roll(x, s):
        s = s % LANES
        return pltpu.roll(x, s, 1) if s else x

    def swap(v, index_bit, weight):
        out = list(v)
        low = (lane // weight) % 2 == 0
        for n in range(len(v)):
            if n & index_bit:
                continue
            a, b = v[n], v[n | index_bit]
            out[n] = jnp.where(low, a, roll(b, weight))
            out[n | index_bit] = jnp.where(low, roll(a, -weight), b)
        return out

    bits = [1 << b for b in range(G.bit_length() - 1)]
    WS = 4 * L

    def swap_slab(v):
        for b in bits:
            v = swap(v, b, WS * b)
        return v

    def swap_source(v):
        for b in bits:
            v = swap(v, b, 2 * b)
        return v

    def lane_x(l):
        return (l // (2 * ny)) % nx * hx + (l // (WS * hy)) % hx

    def lane_y(l):
        return (l // 2) % ny * hy + (l // WS) % hy

    def shift_x(v, step):
        assert hx == 2
        i0 = (lane // (WS * hy)) % 2
        g = (lane // (2 * ny)) % nx
        half, one, all_ = WS * hy, 2 * ny, 2 * ny * (nx - 1)
        flat = roll(v, half)
        if step == 1:
            carry = jnp.where(g < nx - 1, roll(v, half - one), roll(v, half + all_))
            return jnp.where(i0 == 0, flat, carry)
        carry = jnp.where(g > 0, roll(v, half + one), roll(v, half - all_))
        return jnp.where(i0 == 1, flat, carry)

    def shift_y(v, step):
        assert ny == 2
        j0 = (lane // WS) % hy
        g = (lane // 2) % 2
        back = WS * (hy - 1)
        if step == 1:
            carry = jnp.where(g == 0, roll(v, back - 2), roll(v, back + 2))
            return jnp.where(j0 < hy - 1, roll(v, -WS), carry)
        carry = jnp.where(g == 0, roll(v, -back - 2), roll(v, -back + 2))
        return jnp.where(j0 > 0, roll(v, WS), carry)

    def class_rows(q):
        return slice(q * A, (q + 1) * A)

    cells = [(i, j) for i in range(hx) for j in range(hy)]
    M = 2 * A + 16

    def tail_tile(px, i, j):
        out = jnp.zeros((16, LANES), F32)
        for py in (0, 1):
            x, y = 2 * i + px, 2 * j + py
            at = slice(2 * hy * x + y, 2 * hy * x + y + 1)
            out = jnp.where(row16 == py, start_ref[x, y, A:A + 1, :], out)
            out = jnp.where(row16 == 4 + py, coef_high[at, :], out)
            out = jnp.where(row16 == 8 + py, coef_low[at, :], out)
        return out

    zs = coef_ref.shape[1]
    spread = (lax.broadcasted_iota(jnp.int32, (zs, LANES), 1) // (LANES // zs)
              == lax.broadcasted_iota(jnp.int32, (zs, LANES), 0))
    spread = jnp.where(spread, 1.0, 0.0).astype(BF16)
    high = coef_ref[...].astype(BF16)
    low = (coef_ref[...] - high.astype(F32)).astype(BF16)
    coef_high[...] = jnp.dot(high, spread, preferred_element_type=F32)
    coef_low[...] = jnp.dot(low, spread, preferred_element_type=F32)
    for k in range(len(places)):
        load(k).wait()

    def pack(tiles, at):
        v = [swap_slab(t) for t in tiles]
        for s in range(G):
            for half, x in enumerate(swap([v[0][s], v[1][s]], 1, 2)):
                msg[half, s, at, :] = x.astype(BF16)

    for py in (0, 1):
        for r in range(0, A, 16):
            pack([[start_ref[2 * i + px, 2 * j + py, r:r + 16, :] for i, j in cells] for px in (0, 1)],
                 slice(py * A + r, py * A + r + 16))
    pack([[tail_tile(px, i, j) for i, j in cells] for px in (0, 1)], slice(2 * A, M))
    pl.semaphore_wait(barrier, G + 1)
    arrivals = []
    for half in (0, 1):
        arrivals.append([])
        for o in range(1, G):
            s, where = in_plane(o)
            arrivals[half].append(
                remote(msg.at[half, s], rx.at[half, mine], 32 + G * half + o, where))
            arrivals[half][-1].start()
    for half in (0, 1):
        rx[half, mine] = msg[half, slab]

    def dot(a, b):
        return jnp.dot(a, b, preferred_element_type=F32)

    def dot_t(a, b):
        return lax.dot_general(a, b, (((1,), (1,)), ((), ())), preferred_element_type=F32)

    def iota(shape, d):
        return lax.broadcasted_iota(jnp.int32, shape, d)

    def one_hot(hit):
        return jnp.where(hit, 1.0, 0.0).astype(BF16)

    wide2 = 2 * LANES
    src, dst = iota((wide2, 1), 0), iota((1, wide2), 1)

    def column(l, x_step, y_step):
        n = l % LANES
        x, y = (lane_x(n) + x_step) % (hx * nx), (lane_y(n) + y_step) % (hy * ny)
        return ((l // LANES * 2 + l % 2) * (hx * nx) + x) * (hy * ny) + y

    for ref, x_step, y_step in ((XP, 1, 0), (XM, hx * nx - 1, 0), (YP, 0, 1), (YM, 0, hy * ny - 1)):
        ref[...] = one_hot(column(src, 0, 0) == column(dst, x_step, y_step))

    def patch_row(k):
        d, c = k // 8, k % 8
        return c % 2 * D + jnp.where(d < A, c // 2 * A + d, T + c // 2)

    pick = one_hot(patch_row(iota((1, 8 * Q), 1)) == iota((2 * D, 8 * Q), 0))
    p_rows[...] = dot(pick, inverse_ref[...]).astype(BF16)
    pick = one_hot(patch_row(iota((8 * Q, 1), 0)) == iota((8 * Q, 2 * D), 1))
    P[...] = dot(p_rows[...], pick).astype(BF16)

    def packed(k):
        q, d = k // LANES, k % LANES
        return jnp.where(d < A, q * A + d, jnp.where(d == A, T + q, -1))

    cols = one_hot(packed(iota((4 * LANES, 1), 0)) == iota((4 * LANES, D), 1))
    eye = one_hot(iota((D, 1), 0) == iota((D, D), 1))

    def table(blocks):
        U[...] = jnp.zeros_like(U)
        for a, b, m in blocks:
            U[a * A:(a + 1) * A, b * LANES:b * LANES + Q] = m[:A]
            U[T + a:T + a + 1, b * LANES:b * LANES + Q] = m[A:]
        return dot(U[...].astype(BF16), cols).astype(BF16)

    def turned(w):
        return dot_t(eye, w).astype(BF16)

    fx, fy, fz = f_ref[0], f_ref[1], f_ref[2]
    order = ((0, 1, 2, 3, 4), (2, 3, 4, 1, 0))

    def put(k, w):
        for z in (0, 1):
            W[z, :, order[z][k] * D:(order[z][k] + 1) * D] = w[z]

    w = table([(q, q, -m_ref[...]) for q in range(4)])
    put(0, (w, w))
    w = table([(2, 0, fx), (3, 1, fx)])
    w += turned(w)
    put(1, (w, w))
    w = table([(1, 0, fy), (3, 2, fy)])
    w += turned(w)
    put(2, (w, w))
    w = table([(0, 2, fx), (1, 3, fx), (0, 1, fy), (2, 3, fy)])
    w += turned(w)
    put(3, (w, w))
    w = table([(q, q, fz) for q in range(4)])
    put(4, (w, turned(w)))
    S[...] = jnp.zeros_like(S)

    def z_up(c):
        return dot(W[0, :, 4 * D:], c)

    def z_down(c):
        return dot(W[1, :, :D], c)

    def arrive(h):
        for copy in arrivals[h]:
            copy.wait()
        for py in (0, 1):
            for r in range(0, A, 16):
                at = slice(py * A + r, py * A + r + 16)
                v = swap_source([rx[h, n, at, :].astype(F32) for n in range(G)])
                for n in range(G):
                    first = (n % 2 * 2 + py) * A + r
                    R[h, n // 2 + 1 - h, first:first + 16, :] = v[n]
        v = swap_source([rx[h, n, 2 * A:, :].astype(F32) for n in range(G)])
        for z in range(L):
            R[h, z + 1 - h, T:, :] = jnp.where(row16 % 4 < 2, v[2 * z], pltpu.roll(v[2 * z + 1], 2, 0))

    def move(ref, h, idx, d, down, only_tail=False):
        shift = shift_x if d == 0 else shift_y
        bit = 2 >> d
        for q in range(4):
            if q & bit or only_tail:
                continue
            old0 = ref[h, idx, class_rows(q), :]
            old1 = ref[h, idx, class_rows(q + bit), :]
            if down:
                ref[h, idx, class_rows(q), :] = shift(old1, -1)
                ref[h, idx, class_rows(q + bit), :] = old0
            else:
                ref[h, idx, class_rows(q), :] = old1
                ref[h, idx, class_rows(q + bit), :] = shift(old0, 1)
        t = ref[h, idx, T:, :]
        upper = (row16 // bit) % 2 == 1
        if down:
            t = jnp.where(upper, shift(t, -1), t)
        else:
            t = jnp.where(upper, t, shift(t, 1))
        ref[h, idx, T:, :] = jnp.where(upper, pltpu.roll(t, bit, 0), pltpu.roll(t, 16 - bit, 0))

    def first_copy(h):
        return remote(rsb.at[h], rr.at[7, h], 60 + h, ring(1 if h == 0 else -1))

    def enter(h):
        arrive(h)
        end = L if h == 0 else 0
        for idx in [end] + [z + 1 - h for z in range(L) if z + 1 - h != end]:
            for d in (0, 1):
                move(R, h, idx, d, True)
            if idx == end:
                rsb[h] = R[h, end].astype(BF16)
                first_copy(h).start()

    def settle(h):
        first_copy(h).wait()
        R[h, 0 if h == 0 else L] = rr[7, h].astype(F32)
        for idx in range(L + 1):
            t = R[h, idx, T:, :]
            k = t + pltpu.roll(t, 12, 0)
            k = jnp.where((row16 >= 4) & (row16 < 8), k, 1.0)
            s = pltpu.roll(lax.rsqrt(k), 4, 0)
            t = jnp.where(row16 < 4, t, jnp.where(row16 < 8, k, jnp.where(row16 < 12, s, 0.0)))
            R[h, idx, T:, :] = t

    enter(0)
    enter(1)
    settle(0)

    def split(k):
        return k % 2, slice(k // 2 * LANES, (k // 2 + 1) * LANES)

    def block(z, k):
        n = 3 * z + order[z][k]
        return slice(n * D, (n + 1) * D)

    def c_copy(h, base, t, low):
        z, part = split(0 if low else L - 1)
        return remote(B.at[h, block(z, 3), part], cr.at[t, h], t * 4 + h, ring(-1 if low else 1))

    def r_copy(h, base, t, low):
        return remote(rsb.at[h], rr.at[t, h], t * 4 + 2 + h, ring(-1 if low else 1))

    def c2_copy(h, low):
        z, part = split(0 if low else L - 1)
        return remote(B.at[h, block(z, 3), part], cr2.at[h], 62 + h, ring(-1 if low else 1))

    def begin(h, base, t, even, last):
        low = base == 0
        first = 0 if low else 1
        for k in range(L):
            z, part = split(k)
            for q in range(4):
                s = R[h, base + k, T + 8 + q:T + 9 + q, :]
                X[h, z * D + q * A:z * D + (q + 1) * A, part] = (
                    R[h, base + k, class_rows(q), :] * s).astype(BF16)
            t16 = R[h, base + k, T:, :]
            x16 = jnp.where(row16 < 4, t16 * pltpu.roll(t16, 8, 0), 0.0)
            X[h, z * D + T:(z + 1) * D, part] = x16.astype(BF16)

        def solve(z):
            got = dot(P[z * D:(z + 1) * D, :], X[h])
            for p in (0, 1):
                idx = base + 2 * p + z
                part = slice(p * LANES, (p + 1) * LANES)
                end = 2 * p + z == (0 if low else L - 1)
                t16 = R[h, idx, T:, :]
                for q in range(5):
                    if q < 4:
                        at = class_rows(q)
                        s = t16[8 + q:9 + q]
                        k = t16[4 + q:5 + q]
                    else:
                        at = slice(T, D)
                        s = jnp.where(row16 < 4, pltpu.roll(t16, 8, 0), 0.0)
                        k = jnp.where(row16 < 4, pltpu.roll(t16, 12, 0), 0.0)
                    c = got[at, part] * s
                    if not (even and end):
                        S[h, idx, at, :] += c
                    cb = c.astype(BF16)
                    own, cor = block(z, 0).start, block(z, 3).start
                    B[h, own + at.start:own + at.stop, part] = (c * k).astype(BF16)
                    B[h, cor + at.start:cor + at.stop, part] = cb

        def neighbours(z):
            c = B[h, block(z, 3), :]
            t = c[T:]
            r16 = lax.broadcasted_iota(jnp.int32, (16, 2 * LANES), 0)
            xp = dot(jnp.concatenate([c[:2 * A], t], 0), XP[...])
            xm = dot(jnp.concatenate([c[2 * A:T], t], 0), XM[...])
            yp = dot(jnp.concatenate([c[:A], c[2 * A:3 * A], t], 0), YP[...])
            ym = dot(jnp.concatenate([c[A:2 * A], c[3 * A:T], t], 0), YM[...])
            o = block(z, 1).start
            B[h, o:o + 2 * A, :] = xp[:2 * A].astype(BF16)
            B[h, o + 2 * A:o + T, :] = xm[:2 * A].astype(BF16)
            B[h, o + T:o + D, :] = jnp.where(r16 < 2, xp[2 * A:], xm[2 * A:]).astype(BF16)
            o = block(z, 2).start
            B[h, o:o + A, :] = yp[:A].astype(BF16)
            B[h, o + A:o + 2 * A, :] = ym[:A].astype(BF16)
            B[h, o + 2 * A:o + 3 * A, :] = yp[A:2 * A].astype(BF16)
            B[h, o + 3 * A:o + T, :] = ym[A:2 * A].astype(BF16)
            B[h, o + T:o + D, :] = jnp.where(r16 % 2 == 0, yp[2 * A:], ym[2 * A:]).astype(BF16)

        def apply(z):
            acc = dot(W[z], B[h, 3 * z * D:(3 * z + 5) * D, :])
            for p in (0, 1):
                R[h, base + 2 * p + z] += acc[:, p * LANES:(p + 1) * LANES]

        solve(first)
        c_copy(h, base, t, low).start()
        solve(1 - first)
        if last is not None:
            @pl.when(last)
            def _():
                c2_copy(h, not low).start()
        neighbours(first)
        apply(first)
        end = base if low else base + L - 1

        def send_r():
            rsb[h] = R[h, end].astype(BF16)
            r_copy(h, base, t, low).start()

        if last is None:
            send_r()
        else:
            pl.when(jnp.logical_not(last))(send_r)
        neighbours(1 - first)
        apply(1 - first)
        if low:
            acc = z_down(B[h, block(1, 3), :])
            R[h, base + 2] += acc[:, :LANES]
            new, out = acc[:, LANES:], base + L
            R[h, base + 1] += z_up(B[h, block(0, 3), LANES:])
        else:
            acc = z_up(B[h, block(0, 3), :])
            R[h, base + 1] += acc[:, LANES:]
            new, out = acc[:, :LANES], base - 1
            R[h, base + 2] += z_down(B[h, block(1, 3), :LANES])
        R[h, out, :T, :] = new[:T]
        R[h, out, T:T + 4, :] = new[T:T + 4]

    def finish(h, base, t, even, last):
        low = base == 0
        near, out = (base + L - 1, base + L) if low else (base, base - 1)
        c_copy(h, base, t, low).wait()
        c = cr[t, h]
        R[h, near] += z_up(c) if low else z_down(c)
        if even:
            S[h, out] += c.astype(F32)

        def take():
            r_copy(h, base, t, low).wait()
            R[h, out, :T, :] += rr[t, h, :T, :].astype(F32)
            R[h, out, T:T + 4, :] += rr[t, h, T:, :].astype(F32)[:4]

        if last is None:
            take()
        else:
            pl.when(jnp.logical_not(last))(take)

            @pl.when(last)
            def _():
                c2_copy(h, not low).wait()
                other = base if low else base + L - 1
                R[h, other] += z_down(cr2[h]) if low else z_up(cr2[h])

    def between(h, u):
        def shift(d, down):
            for idx in range(L + 1):
                move(R, h, idx, d, down, idx == (L if h == 0 else 0))
            for z in range(L):
                move(S, h, z + 1 - h, d, down)

        @pl.when(lax.rem(u, 2) == 0)
        def _():
            shift(1, False)

        @pl.when(u == 1)
        def _():
            shift(0, False)
            shift(1, True)

    def out_copy(out, got, h, kind, o):
        s, where = in_plane(o)
        return remote(out.at[h, where["gx"] * ny + where["gy"]], got.at[h, slab],
                      64 + (2 * kind + h) * G + o, where)

    def send_out(ref, h, out, got, kind):
        for py in (0, 1):
            for r in range(0, A, 16):
                v = []
                for n in range(G):
                    first = (n % 2 * 2 + py) * A + r
                    v.append(ref[h, n // 2 + 1 - h, first:first + 16, :])
                for n, x in enumerate(swap_source(v)):
                    out[h, n, py * A + r:py * A + r + 16, :] = x.astype(BF16)
        v = []
        for n in range(G):
            t = ref[h, n // 2 + 1 - h, T:, :]
            v.append(pltpu.roll(t, 14, 0) if n % 2 else t)
        for n, x in enumerate(swap_source(v)):
            out[h, n, 2 * A:, :] = x.astype(BF16)
        for o in range(1, G):
            out_copy(out, got, h, kind, o).start()
        got[h, slab] = out[h, mine]

    def body(u, carry):
        begin(0, 0, 2 * u, True, None)

        @pl.when(u > 0)
        def _():
            finish(1, 0, 2 * u - 1, False, None)
            between(1, u - 1)

        pl.when(u == 0)(lambda: settle(1))
        begin(1, 1, 2 * u, True, None)
        finish(0, 0, 2 * u, True, None)
        begin(0, 1, 2 * u + 1, False, u == 3)
        pl.when(u == 3)(lambda: send_out(S, 0, osol, rsol, 0))
        finish(1, 1, 2 * u, True, None)
        begin(1, 0, 2 * u + 1, False, u == 3)
        pl.when(u == 3)(lambda: send_out(S, 1, osol, rsol, 0))
        finish(0, 1, 2 * u + 1, False, u == 3)
        pl.when(u == 3)(lambda: send_out(R, 0, ores, rres, 1))

        @pl.when(u < 3)
        def _():
            between(0, u)
        return carry

    lax.fori_loop(0, 4, body, 0)

    finish(1, 0, 7, False, jnp.bool_(True))
    send_out(R, 1, ores, rres, 1)

    def unpack(got, out):
        def merge(at):
            pairs = [swap([got[0, s, at, :].astype(F32), got[1, s, at, :].astype(F32)], 1, 2)
                     for s in range(G)]
            return [swap_slab([p[px] for p in pairs]) for px in (0, 1)]

        for py in (0, 1):
            for r in range(0, A, 16):
                v = merge(slice(py * A + r, py * A + r + 16))
                for px in (0, 1):
                    for (i, j), x in zip(cells, v[px]):
                        out[2 * i + px, 2 * j + py, r:r + 16, :] = x
        v = merge(slice(2 * A, M))
        for px in (0, 1):
            for (i, j), x in zip(cells, v[px]):
                for py in (0, 1):
                    out[2 * i + px, 2 * j + py, A:A + 1, :] = x[py:py + 1]

    n = len(places)
    for h in (0, 1):
        for o in range(1, G):
            out_copy(osol, rsol, h, 0, o).wait()
    unpack(rsol, sol_ref)
    for k in range(n):
        store(sol_ref, sol_out, k, 0).start()
    for h in (0, 1):
        for o in range(1, G):
            out_copy(ores, rres, h, 1, o).wait()
    unpack(rres, res_ref)
    for k in range(n):
        store(res_ref, res_out, k, n).start()
    for k in range(n):
        store(sol_ref, sol_out, k, 0).wait()
        store(res_ref, res_out, k, n).wait()


def in_slabs(sizes, right_side, cell_coef, cell_matrix, face_coupling, patch_inverse):
    Q = cell_matrix.shape[0]
    X, Y, Z = cell_coef.shape
    lanes = right_side.shape[3]
    nx, ny, nz = sizes
    G = nx * ny
    D = 4 * (Q - 1) + 16
    coef = cell_coef.reshape(X * Y, Z)
    V = pltpu.VMEM
    half = (D, LANES)
    side = (2 * LANES, 2 * LANES)
    block = (X, Y, Q, lanes)
    piece = (2, G, 2 * (Q - 1) + 16, LANES)
    scratch = [
        V(block, F32), V(block, F32), V(block, F32), V((X * Y, lanes), F32), V((X * Y, lanes), F32),
        V(piece, BF16), V(piece, BF16),
        V((2, 5, *half), F32), V((2, 5, *half), F32),
        V((2, 2 * D, 2 * LANES), BF16), V((2, 8 * D, 2 * LANES), BF16),
        V((2, D, 5 * D), BF16), V((2 * D, 2 * D), BF16),
        V(side, BF16), V(side, BF16), V(side, BF16), V(side, BF16),
        V((D, 4 * LANES), F32), V((2 * D, 8 * Q), BF16),
        V((8, 2, *half), BF16), V((8, 2, *half), BF16), V((2, *half), BF16), V((2, *half), BF16),
        V(piece, BF16), V(piece, BF16), V(piece, BF16), V(piece, BF16),
        pltpu.SemaphoreType.DMA((96,)), pltpu.SemaphoreType.DMA((96,)),
        pltpu.SemaphoreType.DMA((X * Y,)), pltpu.SemaphoreType.DMA((2 * X * Y,)),
    ]
    vmem = pl.BlockSpec(memory_space=pltpu.VMEM)
    sol, res = pl.pallas_call(
        functools.partial(slab_kernel, sizes, (Q, nx, ny, nz, X // 2, Y // 2)),
        out_shape=[jax.ShapeDtypeStruct(right_side.shape, F32)] * 2,
        in_specs=[pl.BlockSpec(memory_space=pl.ANY)] + [vmem] * 4,
        out_specs=[pl.BlockSpec(memory_space=pl.ANY)] * 2,
        scratch_shapes=scratch,
        compiler_params=pltpu.CompilerParams(
            collective_id=0, has_side_effects=True, vmem_limit_bytes=60 * 1024 * 1024),
    )(right_side, coef, patch_inverse, cell_matrix, face_coupling)
    return sol, res


def on_device(sizes, right_side, cell_coef, cell_matrix, face_coupling, patch_inverse):
    X, Y, Z = cell_coef.shape
    form = in_slabs if fits_slabs(sizes, cell_matrix.shape[0], X, Y, Z, right_side.shape[3]) else in_blocks
    return form(sizes, right_side, cell_coef, cell_matrix, face_coupling, patch_inverse)


def solution(mesh):
    sizes = tuple(mesh.shape[a] for a in AXES)
    placed = (P(None, "gx", "gy", "gz"), P("gx", "gy", "gz"), P(), P(), P())
    return jax.shard_map(
        functools.partial(on_device, sizes),
        mesh=mesh,
        in_specs=placed,
        out_specs=(P(None, "gx", "gy", "gz"), P(None, "gx", "gy", "gz")),
        check_vma=False,
    )
```

```python
import functools
import jax
import jax.numpy as jnp
from jax import lax
from jax.experimental import pallas as pl
from jax.experimental.pallas import tpu as pltpu
from jax.sharding import PartitionSpec as P

AXES = ("gx", "gy", "gz")
MESH = pl.DeviceIdType.MESH
F32, BF16 = jnp.float32, jnp.bfloat16
LANES = 128


def class_pairs(d):
    bit = 4 >> d
    return [(c, c + bit) for c in range(8) if not c & bit]


def block_kernel(sizes, dims, start_ref, inverse_ref, w_ref, sol_ref, res_ref,
           R, S2, Sx, scaled, corr, ccorr, Xx, Xy, Xz,
           fx, fxe, fy, fz, fxes, fys, fzs, mxr, mxe, mxs, myr, mys, mzr,
           mxr_s, mxs_s, myr_s, mys_s, mzr_s, p_rows, p_ref, send_sem, recv_sem):
    D, Q, nr, ni, njh = dims
    w = 2 * nr
    A = Q // 16 * 16
    tiles = [(i, jh) for i in range(ni) for jh in range(njh)]
    C = ni * njh * LANES
    half = njh * LANES
    lane = lax.broadcasted_iota(jnp.int32, (D, LANES), 1)
    jlo0 = (lane // nr) % 2 == 0
    piece = lane // w

    me = [lax.axis_index(a) for a in AXES]

    def neighbour(d, step):
        n = sizes[d]
        return {AXES[d]: lax.rem(me[d] + step + n, n)}

    barrier = pltpu.get_barrier_semaphore()
    for d in range(3):
        for step in (1, -1):
            pl.semaphore_signal(barrier, inc=1, device_id=neighbour(d, step), device_id_type=MESH)

    def rows(c):
        return slice(c * D, (c + 1) * D)

    def cols(i, jh):
        t = i * njh + jh
        return slice(t * LANES, (t + 1) * LANES)

    def get(ref, c):
        return {t: ref[c, :, cols(*t)].astype(F32) for t in tiles}

    def roll(x, s):
        s = s % LANES
        return pltpu.roll(x, s, 1) if s else x

    for c in range(0, 8, 2):
        ox, oy = c // 4, c // 2 % 2
        for i, jh in tiles:
            a = start_ref[2 * i + ox, 4 * jh + oy]
            b = start_ref[2 * i + ox, 4 * jh + 2 + oy]
            R[c, :, cols(i, jh)] = jnp.where(jlo0, a, roll(b, nr))
            R[c + 1, :, cols(i, jh)] = jnp.where(jlo0, roll(a, -nr), b)
    S2[...] = jnp.zeros_like(S2)
    pl.semaphore_wait(barrier, 6)

    def pack_y(ref, last):
        out = []
        for p in class_pairs(1):
            c = p[1] if last else p[0]
            jh = njh - 1 if last else 0
            t0 = ref[c, :, cols(0, jh)].astype(F32)
            t1 = ref[c, :, cols(1, jh)].astype(F32)
            if last:
                out.append(jnp.where(jlo0, roll(t1, -nr), t0))
            else:
                out.append(jnp.where(jlo0, t0, roll(t1, nr)))
        return jnp.stack(out, 0)

    def pack_z(ref, last):
        acc = jnp.zeros((D, LANES), F32)
        n = 0
        for p in class_pairs(2):
            c = p[1] if last else p[0]
            for t in tiles:
                x = ref[c, :, cols(*t)].astype(F32)
                x = roll(x, w * (n + 1) if last else w * n)
                acc = jnp.where(piece == n, x, acc)
                n += 1
        return acc

    def shifted(d, step, have, halo, pc):
        out = {}
        for i, jh in tiles:
            if d == 0:
                at = i + step
                if 0 <= at < ni:
                    new = have[at, jh]
                else:
                    new = halo(slice(jh * LANES, (jh + 1) * LANES))
            elif d == 1:
                at = jh + step
                if 0 <= at < njh:
                    other = roll(have[i, at], step * nr)
                else:
                    other = halo(slice(0, LANES))
                    if i == 0:
                        other = roll(other, step * nr)
                cur = roll(have[i, jh], -step * nr)
                new = jnp.where(jlo0, cur, other) if step == 1 else jnp.where(jlo0, other, cur)
            else:
                n = pc * len(tiles) + i * njh + jh
                h = halo(slice(0, LANES))
                if step == 1:
                    new = jnp.where(lane >= LANES - w, roll(h, LANES - w - w * n),
                                    roll(have[i, jh], -w))
                else:
                    new = jnp.where(lane < w, roll(h, -w * n), roll(have[i, jh], w))
            out[i, jh] = new
        return out

    def read_x(t, last, pc):
        first = lax.broadcasted_iota(jnp.int32, (D - A, LANES), 0) == 0

        def halo(c):
            tail = fxe[t, last, :, c].astype(F32)[pc:pc + 1]
            return jnp.concatenate(
                [fx[t, last, pc, :, c].astype(F32), jnp.where(first, tail, 0.0)], 0)
        return halo

    def read_y(ref, *at):
        return lambda c: ref[(*at, slice(None), c)].astype(F32)

    def remote(src, dst, k, d, step):
        return pltpu.make_async_remote_copy(
            src_ref=src, dst_ref=dst, send_sem=send_sem.at[k], recv_sem=recv_sem.at[k],
            device_id=neighbour(d, step), device_id_type=MESH)

    def move(d, down, copies, halo, beside=None):
        for copy in copies:
            copy.start()
        if beside is not None:
            beside()
        for copy in copies:
            copy.wait()
        for pc, (c0, c1) in enumerate(class_pairs(d)):
            old0, old1 = get(R, c0), get(R, c1)
            if down:
                new0, new1 = shifted(d, -1, old1, halo(pc), pc), old0
            else:
                new0, new1 = old1, shifted(d, 1, old0, halo(pc), pc)
            for t in tiles:
                R[c0, :, cols(*t)] = new0[t]
                R[c1, :, cols(*t)] = new1[t]

    def move_x(down, at, beside=None):
        part = slice((ni - 1) * half, ni * half) if down else slice(0, half)
        cs = slice(4, 8) if down else slice(0, 4)
        mxr_s[...] = R[cs, :A, part].astype(BF16)
        step = 1 if down else -1
        copies = [remote(mxr_s, mxr.at[at], 72 + at, 0, step),
                  remote(R.at[cs, A:A + 8, part], mxe.at[at], 74 + at, 0, step)]
        zeros = jnp.zeros((D - A - 8, LANES), F32)

        def halo(pc):
            return lambda c: jnp.concatenate(
                [mxr[at, pc, :, c].astype(F32), mxe[at, pc, :, c], zeros], 0)
        move(0, down, copies, halo, beside)

    def move_y(down, u):
        myr_s[...] = pack_y(R, down)
        move(1, down, [remote(myr_s, myr.at[u], 64 + u, 1, 1 if down else -1)],
             lambda pc: read_y(myr, u, pc))

    def move_z(down, t):
        mzr_s[...] = pack_z(R, down)
        move(2, down, [remote(mzr_s, mzr.at[t], 48 + t, 2, 1 if down else -1)],
             lambda pc: read_y(mzr, t))

    def sol_y(u):
        return remote(mys_s, mys.at[lax.div(u, 2)], 56 + lax.div(u, 2), 1, -1)

    def sol_x():
        return remote(mxs_s, mxs, 58, 0, -1)

    def pair(ref, q):
        return ref[2 * q:2 * q + 2].reshape(2 * D, C)

    def lessen(q, acc):
        R[2 * q:2 * q + 2] -= acc.reshape(2, D, C)

    def dot(a, b):
        return jnp.dot(a, b, preferred_element_type=F32)

    def colour(t, v, sb):
        for c in range(8):
            s = R[c, Q:Q + 1, :]
            scaled[c] = (s * R[c]).astype(BF16)
        copies = [[None, None] for _ in range(3)]
        extra = [None, None]
        line = lax.broadcasted_iota(jnp.int32, (16, half), 0)
        for n in range(ni):
            part = slice(n * half, (n + 1) * half)
            solved = dot(p_ref[...], scaled[:, :, part].reshape(8 * D, half))
            for c in range(8):
                s = R[c, Q:Q + 1, part]
                k = R[c, Q + 1:Q + 2, part]
                got = s * solved[rows(c), :]
                if v == 1:
                    S2[sb, c, :, part] += got
                corr[c, :, part] = got.astype(BF16)
                ccorr[c, :, part] = (k * got).astype(BF16)
            for last in (0, 1):
                if n != (ni - 1 if last else 0):
                    continue
                step = 1 if last else -1
                tail = jnp.zeros((16, half), F32)
                for pc in range(4):
                    row = corr[4 * last + pc, A:, part].astype(F32)[:1]
                    tail = jnp.where(line == pc, row, tail)
                fxes[last] = tail.astype(BF16)
                copies[0][last] = remote(corr.at[4 * last:4 * last + 4, :A, part], fx.at[t, last],
                                         t * 6 + last, 0, step)
                copies[0][last].start()
                extra[last] = remote(fxes.at[last], fxe.at[t, last], 80 + 2 * t + last, 0, step)
                extra[last].start()
        for last in (0, 1):
            fzs[last] = pack_z(corr, last).astype(BF16)
            copies[2][last] = remote(fzs.at[last], fz.at[t, last], t * 6 + 4 + last, 2, 1 if last else -1)
            copies[2][last].start()
        for last in (0, 1):
            fys[last] = pack_y(corr, last).astype(BF16)
            copies[1][last] = remote(fys.at[last], fy.at[t, last], t * 6 + 2 + last, 1, 1 if last else -1)
            copies[1][last].start()
        for q in range(4):
            acc = dot(w_ref[0], pair(ccorr, q))
            acc += dot(w_ref[1], pair(corr, q))
            acc += dot(w_ref[3 if q // 2 == 0 else 4], pair(corr, q ^ 2))
            acc += dot(w_ref[5 if q % 2 == 0 else 6], pair(corr, q ^ 1))
            lessen(q, acc)

        def fill(d, X, halo0, halo1):
            for pc, (c0, c1) in enumerate(class_pairs(d)):
                new0 = shifted(d, 1, get(corr, c0), halo0(pc), pc)
                new1 = shifted(d, -1, get(corr, c1), halo1(pc), pc)
                for at in tiles:
                    X[c0, :, cols(*at)] = new0[at].astype(BF16)
                    X[c1, :, cols(*at)] = new1[at].astype(BF16)

        for copy in copies[2]:
            copy.wait()
        fill(2, Xz, lambda pc: read_y(fz, t, 0), lambda pc: read_y(fz, t, 1))
        if v == 0:
            for c0, c1 in class_pairs(2):
                S2[sb, c0] += corr[c1].astype(F32)
                S2[sb, c1] += Xz[c0].astype(F32)
        for copy in copies[1]:
            copy.wait()
        fill(1, Xy, lambda pc: read_y(fy, t, 0, pc), lambda pc: read_y(fy, t, 1, pc))
        for q in range(4):
            acc = dot(w_ref[2], pair(Xz, q))
            acc += dot(w_ref[6 if q % 2 == 0 else 5], pair(Xy, q ^ 1))
            lessen(q, acc)
        for copy in copies[0] + extra:
            copy.wait()
        fill(0, Xx, lambda pc: read_x(t, 0, pc), lambda pc: read_x(t, 1, pc))
        for q in range(4):
            lessen(q, dot(w_ref[4 if q // 2 == 0 else 3], pair(Xx, q ^ 2)))

    def class_order():
        r = lax.broadcasted_iota(jnp.int32, (D, 8 * Q), 0)
        k = lax.broadcasted_iota(jnp.int32, (D, 8 * Q), 1)
        for c in range(8):
            pick = jnp.where((k == r * 8 + c) & (r < Q), 1.0, 0.0).astype(BF16)
            p_rows[c * D:(c + 1) * D, :] = dot(pick, inverse_ref[...]).astype(BF16)
        k = lax.broadcasted_iota(jnp.int32, (8 * Q, 8 * D), 0)
        r = lax.broadcasted_iota(jnp.int32, (8 * Q, 8 * D), 1)
        q = r % D
        pick = jnp.where((k == q * 8 + r // D) & (q < Q), 1.0, 0.0).astype(BF16)
        p_ref[...] = dot(p_rows[...], pick).astype(BF16)

    def body(u, carry):
        @pl.when(u == 0)
        def _():
            move_x(True, 0, class_order)

        @pl.when(u == 2)
        def _():
            move_x(False, 1)
            for c in range(8):
                Sx[c] = S2[1, c]
            mxs_s[...] = S2[1, :4, :, :half].astype(BF16)
            sol_x().start()
            S2[1] = jnp.zeros_like(Sx)

        @pl.when(lax.rem(u, 2) == 0)
        def _():
            S2[0] = jnp.zeros_like(Sx)
            move_y(True, u)

        @pl.when(lax.rem(u, 2) == 1)
        def _():
            move_y(False, u)
            mys_s[...] = pack_y(S2.at[0], False).astype(BF16)
            sol_y(u).start()

        for v in (0, 1):
            t = 2 * u + v
            move_z(v == 0, t)
            colour(t, v, lax.rem(u, 2))

        @pl.when(lax.rem(u, 2) == 1)
        def _():
            sol_y(u).wait()
            for pc, (c0, c1) in enumerate(class_pairs(1)):
                S2[1, c0] += S2[0, c1]
                new = shifted(1, 1, get(S2.at[0], c0), read_y(mys, lax.div(u, 2), pc), pc)
                for at in tiles:
                    S2[1, c1, :, cols(*at)] += new[at]
        return carry

    lax.fori_loop(0, 4, body, 0)
    sol_x().wait()
    for pc, (c0, c1) in enumerate(class_pairs(0)):
        S2[1, c0] += Sx[c1]
        new = shifted(0, 1, get(Sx, c0), read_y(mxs, pc), pc)
        for at in tiles:
            S2[1, c1, :, cols(*at)] += new[at]

    for ref, out in ((S2.at[1], sol_ref), (R, res_ref)):
        for c in range(0, 8, 2):
            ox, oy = c // 4, c // 2 % 2
            for i, jh in tiles:
                x0 = ref[c, :, cols(i, jh)]
                x1 = ref[c + 1, :, cols(i, jh)]
                out[2 * i + ox, 4 * jh + oy] = jnp.where(jlo0, x0, roll(x1, nr))
                out[2 * i + ox, 4 * jh + 2 + oy] = jnp.where(jlo0, roll(x0, -nr), x1)


def in_blocks(sizes, right_side, cell_coef, cell_matrix, face_coupling, patch_inverse):
    Q = cell_matrix.shape[0]
    X, Y, Z = cell_coef.shape
    lanes = right_side.shape[3]
    nr = lanes // Z
    D = -(-(Q + 2) // 16) * 16
    ni, njh = X // 2, Y // 4
    assert lanes == LANES and ni == 2 and 4 * ni * njh * 2 * nr == LANES
    C = ni * njh * LANES
    coef = jnp.repeat(cell_coef, nr, axis=2)
    extra = jnp.stack([lax.rsqrt(coef), coef], 2)
    start = jnp.concatenate(
        [jnp.transpose(right_side, (1, 2, 0, 3)), extra, jnp.zeros((X, Y, D - Q - 2, lanes), F32)], 2)
    def padded(m):
        return jnp.pad(m, ((0, D - Q), (0, D - Q)))

    zero = jnp.zeros((D, D), F32)

    def both(a, b, c, d):
        return jnp.concatenate([jnp.concatenate([a, b], 1), jnp.concatenate([c, d], 1)], 0)

    m = padded(cell_matrix)
    f = [-padded(face_coupling[d]) for d in range(3)]
    ft = [x.T for x in f]
    mats = jnp.stack([
        both(m, zero, zero, m),
        both(zero, f[2], ft[2], zero),
        both(zero, ft[2], f[2], zero),
        both(f[0], zero, zero, f[0]),
        both(ft[0], zero, zero, ft[0]),
        both(f[1], zero, zero, f[1]),
        both(ft[1], zero, zero, ft[1]),
    ]).astype(BF16)
    half = njh * LANES
    V = pltpu.VMEM
    A = Q // 16 * 16
    assert Q == A + 1
    whole = (8, D, C)
    scratch = [
        V(whole, F32), V((2, *whole), F32), V(whole, F32), V(whole, BF16), V(whole, BF16), V(whole, BF16),
        V(whole, BF16), V(whole, BF16), V(whole, BF16),
        V((8, 2, 4, A, half), BF16), V((8, 2, 16, half), BF16),
        V((8, 2, 4, D, LANES), BF16), V((8, 2, D, LANES), BF16),
        V((2, 16, half), BF16), V((2, 4, D, LANES), BF16), V((2, D, LANES), BF16),
        V((2, 4, A, half), BF16), V((2, 4, 8, half), F32), V((4, D, half), BF16),
        V((4, 4, D, LANES), F32), V((2, 4, D, LANES), BF16), V((8, D, LANES), F32),
        V((4, A, half), BF16), V((4, D, half), BF16),
        V((4, D, LANES), F32), V((4, D, LANES), BF16), V((D, LANES), F32),
        V((8 * D, 8 * Q), BF16), V((8 * D, 8 * D), BF16),
        pltpu.SemaphoreType.DMA((96,)), pltpu.SemaphoreType.DMA((96,)),
    ]
    vmem = pl.BlockSpec(memory_space=pltpu.VMEM)
    sol, res = pl.pallas_call(
        functools.partial(block_kernel, sizes, (D, Q, nr, ni, njh)),
        out_shape=[jax.ShapeDtypeStruct((X, Y, D, lanes), F32)] * 2,
        in_specs=[vmem] * 3,
        out_specs=[vmem] * 2,
        scratch_shapes=scratch,
        compiler_params=pltpu.CompilerParams(
            collective_id=0, has_side_effects=True, vmem_limit_bytes=46 * 1024 * 1024),
    )(start, patch_inverse, mats)
    return tuple(jnp.transpose(x[:, :, :Q], (2, 0, 1, 3)) for x in (sol, res))


def fits_slabs(sizes, Q, X, Y, Z, lanes):
    group = sizes[0] * sizes[1]
    layers = Z // group
    return (lanes == LANES and Q % 16 == 1 and layers == 4 and Z == layers * group
            and (X // 2) * (Y // 2) == group and lanes // Z == 4 and 2 * layers == group
            and X % 2 == 0 and Y % 2 == 0)


def slab_kernel(sizes, dims, start_ref, coef_ref, inverse_ref, m_ref, f_ref, sol_ref, res_ref,
                coef_high, coef_low, msg, rx, R, S, X, B, W, P, XP, XM, YP, YM, U, p_rows,
                cr, rr, cr2, rsb, osol, ores, rsol, rres, send_sem, recv_sem):
    Q, nx, ny, nz, hx, hy = dims
    G = nx * ny
    L = 4
    A = Q - 1
    T = 4 * A
    D = T + 16
    wide = 1
    while wide * wide < nx:
        wide += 1
    lane = lax.broadcasted_iota(jnp.int32, (1, LANES), 1)
    row16 = lax.broadcasted_iota(jnp.int32, (16, LANES), 0)

    gx, gy, gz = [lax.axis_index(a) for a in AXES]
    mine = gx * ny + gy

    def snake(p):
        row = p // wide
        col = p % wide
        return row * wide + col + (row % 2) * (wide - 1 - 2 * col)

    def flip(p, plane):
        return p + (plane % 2) * (nx - 1 - 2 * p)

    slab = flip(snake(gx), gz) * ny + gy

    def device(plane, s):
        return {"gx": snake(flip(s // ny, plane)), "gy": s % ny, "gz": plane}

    def ring(step):
        g = lax.rem(gz * G + slab + step + nz * G, nz * G)
        return device(g // G, g % G)

    def in_plane(o):
        s = lax.rem(slab + o, G)
        return s, device(gz, s)

    barrier = pltpu.get_barrier_semaphore()
    for o in range(1, G):
        pl.semaphore_signal(barrier, inc=1, device_id=in_plane(o)[1], device_id_type=MESH)
    for step in (1, -1):
        pl.semaphore_signal(barrier, inc=1, device_id=ring(step), device_id_type=MESH)

    def remote(src, dst, k, where):
        return pltpu.make_async_remote_copy(
            src_ref=src, dst_ref=dst, send_sem=send_sem.at[k], recv_sem=recv_sem.at[k],
            device_id=where, device_id_type=MESH)

    def roll(x, s):
        s = s % LANES
        return pltpu.roll(x, s, 1) if s else x

    def swap(v, index_bit, weight):
        out = list(v)
        low = (lane // weight) % 2 == 0
        for n in range(len(v)):
            if n & index_bit:
                continue
            a, b = v[n], v[n | index_bit]
            out[n] = jnp.where(low, a, roll(b, weight))
            out[n | index_bit] = jnp.where(low, roll(a, -weight), b)
        return out

    bits = [1 << b for b in range(G.bit_length() - 1)]
    WS = 4 * L

    def swap_slab(v):
        for b in bits:
            v = swap(v, b, WS * b)
        return v

    def swap_source(v):
        for b in bits:
            v = swap(v, b, 2 * b)
        return v

    def lane_x(l):
        return (l // (2 * ny)) % nx * hx + (l // (WS * hy)) % hx

    def lane_y(l):
        return (l // 2) % ny * hy + (l // WS) % hy

    def shift_x(v, step):
        assert hx == 2
        i0 = (lane // (WS * hy)) % 2
        g = (lane // (2 * ny)) % nx
        half, one, all_ = WS * hy, 2 * ny, 2 * ny * (nx - 1)
        flat = roll(v, half)
        if step == 1:
            carry = jnp.where(g < nx - 1, roll(v, half - one), roll(v, half + all_))
            return jnp.where(i0 == 0, flat, carry)
        carry = jnp.where(g > 0, roll(v, half + one), roll(v, half - all_))
        return jnp.where(i0 == 1, flat, carry)

    def shift_y(v, step):
        assert ny == 2
        j0 = (lane // WS) % hy
        g = (lane // 2) % 2
        back = WS * (hy - 1)
        if step == 1:
            carry = jnp.where(g == 0, roll(v, back - 2), roll(v, back + 2))
            return jnp.where(j0 < hy - 1, roll(v, -WS), carry)
        carry = jnp.where(g == 0, roll(v, -back - 2), roll(v, -back + 2))
        return jnp.where(j0 > 0, roll(v, WS), carry)

    def class_rows(q):
        return slice(q * A, (q + 1) * A)

    cells = [(i, j) for i in range(hx) for j in range(hy)]
    M = 2 * A + 16

    def tail_tile(px, i, j):
        out = jnp.zeros((16, LANES), F32)
        for py in (0, 1):
            x, y = 2 * i + px, 2 * j + py
            at = slice(2 * hy * x + y, 2 * hy * x + y + 1)
            out = jnp.where(row16 == py, start_ref[x, y, A:A + 1, :], out)
            out = jnp.where(row16 == 4 + py, coef_high[at, :], out)
            out = jnp.where(row16 == 8 + py, coef_low[at, :], out)
        return out

    zs = coef_ref.shape[1]
    spread = (lax.broadcasted_iota(jnp.int32, (zs, LANES), 1) // (LANES // zs)
              == lax.broadcasted_iota(jnp.int32, (zs, LANES), 0))
    spread = jnp.where(spread, 1.0, 0.0).astype(BF16)
    high = coef_ref[...].astype(BF16)
    low = (coef_ref[...] - high.astype(F32)).astype(BF16)
    coef_high[...] = jnp.dot(high, spread, preferred_element_type=F32)
    coef_low[...] = jnp.dot(low, spread, preferred_element_type=F32)

    def pack(tiles, at):
        v = [swap_slab(t) for t in tiles]
        for s in range(G):
            for half, x in enumerate(swap([v[0][s], v[1][s]], 1, 2)):
                msg[half, s, at, :] = x.astype(BF16)

    for py in (0, 1):
        for r in range(0, A, 16):
            pack([[start_ref[2 * i + px, 2 * j + py, r:r + 16, :] for i, j in cells] for px in (0, 1)],
                 slice(py * A + r, py * A + r + 16))
    pack([[tail_tile(px, i, j) for i, j in cells] for px in (0, 1)], slice(2 * A, M))
    pl.semaphore_wait(barrier, G + 1)
    arrivals = []
    for half in (0, 1):
        arrivals.append([])
        for o in range(1, G):
            s, where = in_plane(o)
            arrivals[half].append(
                remote(msg.at[half, s], rx.at[half, mine], 32 + G * half + o, where))
            arrivals[half][-1].start()
    for half in (0, 1):
        rx[half, mine] = msg[half, slab]

    def dot(a, b):
        return jnp.dot(a, b, preferred_element_type=F32)

    def dot_t(a, b):
        return lax.dot_general(a, b, (((1,), (1,)), ((), ())), preferred_element_type=F32)

    def iota(shape, d):
        return lax.broadcasted_iota(jnp.int32, shape, d)

    def one_hot(hit):
        return jnp.where(hit, 1.0, 0.0).astype(BF16)

    wide2 = 2 * LANES
    src, dst = iota((wide2, 1), 0), iota((1, wide2), 1)

    def column(l, x_step, y_step):
        n = l % LANES
        x, y = (lane_x(n) + x_step) % (hx * nx), (lane_y(n) + y_step) % (hy * ny)
        return ((l // LANES * 2 + l % 2) * (hx * nx) + x) * (hy * ny) + y

    for ref, x_step, y_step in ((XP, 1, 0), (XM, hx * nx - 1, 0), (YP, 0, 1), (YM, 0, hy * ny - 1)):
        ref[...] = one_hot(column(src, 0, 0) == column(dst, x_step, y_step))

    def patch_row(k):
        d, c = k // 8, k % 8
        return c % 2 * D + jnp.where(d < A, c // 2 * A + d, T + c // 2)

    pick = one_hot(patch_row(iota((1, 8 * Q), 1)) == iota((2 * D, 8 * Q), 0))
    p_rows[...] = dot(pick, inverse_ref[...]).astype(BF16)
    pick = one_hot(patch_row(iota((8 * Q, 1), 0)) == iota((8 * Q, 2 * D), 1))
    P[...] = dot(p_rows[...], pick).astype(BF16)

    def packed(k):
        q, d = k // LANES, k % LANES
        return jnp.where(d < A, q * A + d, jnp.where(d == A, T + q, -1))

    cols = one_hot(packed(iota((4 * LANES, 1), 0)) == iota((4 * LANES, D), 1))
    eye = one_hot(iota((D, 1), 0) == iota((D, D), 1))

    def table(blocks):
        U[...] = jnp.zeros_like(U)
        for a, b, m in blocks:
            U[a * A:(a + 1) * A, b * LANES:b * LANES + Q] = m[:A]
            U[T + a:T + a + 1, b * LANES:b * LANES + Q] = m[A:]
        return dot(U[...].astype(BF16), cols).astype(BF16)

    def turned(w):
        return dot_t(eye, w).astype(BF16)

    fx, fy, fz = f_ref[0], f_ref[1], f_ref[2]
    order = ((0, 1, 2, 3, 4), (2, 3, 4, 1, 0))

    def put(k, w):
        for z in (0, 1):
            W[z, :, order[z][k] * D:(order[z][k] + 1) * D] = w[z]

    w = table([(q, q, -m_ref[...]) for q in range(4)])
    put(0, (w, w))
    w = table([(2, 0, fx), (3, 1, fx)])
    w += turned(w)
    put(1, (w, w))
    w = table([(1, 0, fy), (3, 2, fy)])
    w += turned(w)
    put(2, (w, w))
    w = table([(0, 2, fx), (1, 3, fx), (0, 1, fy), (2, 3, fy)])
    w += turned(w)
    put(3, (w, w))
    w = table([(q, q, fz) for q in range(4)])
    put(4, (w, turned(w)))
    S[...] = jnp.zeros_like(S)

    def z_up(c):
        return dot(W[0, :, 4 * D:], c)

    def z_down(c):
        return dot(W[1, :, :D], c)

    def arrive(h):
        for copy in arrivals[h]:
            copy.wait()
        for py in (0, 1):
            for r in range(0, A, 16):
                at = slice(py * A + r, py * A + r + 16)
                v = swap_source([rx[h, n, at, :].astype(F32) for n in range(G)])
                for n in range(G):
                    first = (n % 2 * 2 + py) * A + r
                    R[h, n // 2 + 1 - h, first:first + 16, :] = v[n]
        v = swap_source([rx[h, n, 2 * A:, :].astype(F32) for n in range(G)])
        for z in range(L):
            R[h, z + 1 - h, T:, :] = jnp.where(row16 % 4 < 2, v[2 * z], pltpu.roll(v[2 * z + 1], 2, 0))

    def move(ref, h, idx, d, down, only_tail=False):
        shift = shift_x if d == 0 else shift_y
        bit = 2 >> d
        for q in range(4):
            if q & bit or only_tail:
                continue
            old0 = ref[h, idx, class_rows(q), :]
            old1 = ref[h, idx, class_rows(q + bit), :]
            if down:
                ref[h, idx, class_rows(q), :] = shift(old1, -1)
                ref[h, idx, class_rows(q + bit), :] = old0
            else:
                ref[h, idx, class_rows(q), :] = old1
                ref[h, idx, class_rows(q + bit), :] = shift(old0, 1)
        t = ref[h, idx, T:, :]
        upper = (row16 // bit) % 2 == 1
        if down:
            t = jnp.where(upper, shift(t, -1), t)
        else:
            t = jnp.where(upper, t, shift(t, 1))
        ref[h, idx, T:, :] = jnp.where(upper, pltpu.roll(t, bit, 0), pltpu.roll(t, 16 - bit, 0))

    def first_copy(h):
        return remote(rsb.at[h], rr.at[7, h], 60 + h, ring(1 if h == 0 else -1))

    def enter(h):
        arrive(h)
        end = L if h == 0 else 0
        for idx in [end] + [z + 1 - h for z in range(L) if z + 1 - h != end]:
            for d in (0, 1):
                move(R, h, idx, d, True)
            if idx == end:
                rsb[h] = R[h, end].astype(BF16)
                first_copy(h).start()

    def settle(h):
        first_copy(h).wait()
        R[h, 0 if h == 0 else L] = rr[7, h].astype(F32)
        for idx in range(L + 1):
            t = R[h, idx, T:, :]
            k = t + pltpu.roll(t, 12, 0)
            k = jnp.where((row16 >= 4) & (row16 < 8), k, 1.0)
            s = pltpu.roll(lax.rsqrt(k), 4, 0)
            t = jnp.where(row16 < 4, t, jnp.where(row16 < 8, k, jnp.where(row16 < 12, s, 0.0)))
            R[h, idx, T:, :] = t

    enter(0)
    enter(1)
    settle(0)

    def split(k):
        return k % 2, slice(k // 2 * LANES, (k // 2 + 1) * LANES)

    def block(z, k):
        n = 3 * z + order[z][k]
        return slice(n * D, (n + 1) * D)

    def c_copy(h, base, t, low):
        z, part = split(0 if low else L - 1)
        return remote(B.at[h, block(z, 3), part], cr.at[t, h], t * 4 + h, ring(-1 if low else 1))

    def r_copy(h, base, t, low):
        return remote(rsb.at[h], rr.at[t, h], t * 4 + 2 + h, ring(-1 if low else 1))

    def c2_copy(h, low):
        z, part = split(0 if low else L - 1)
        return remote(B.at[h, block(z, 3), part], cr2.at[h], 62 + h, ring(-1 if low else 1))

    def begin(h, base, t, even, last):
        low = base == 0
        first = 0 if low else 1
        for k in range(L):
            z, part = split(k)
            for q in range(4):
                s = R[h, base + k, T + 8 + q:T + 9 + q, :]
                X[h, z * D + q * A:z * D + (q + 1) * A, part] = (
                    R[h, base + k, class_rows(q), :] * s).astype(BF16)
            t16 = R[h, base + k, T:, :]
            x16 = jnp.where(row16 < 4, t16 * pltpu.roll(t16, 8, 0), 0.0)
            X[h, z * D + T:(z + 1) * D, part] = x16.astype(BF16)

        def solve(z):
            got = dot(P[z * D:(z + 1) * D, :], X[h])
            for p in (0, 1):
                idx = base + 2 * p + z
                part = slice(p * LANES, (p + 1) * LANES)
                end = 2 * p + z == (0 if low else L - 1)
                t16 = R[h, idx, T:, :]
                for q in range(5):
                    if q < 4:
                        at = class_rows(q)
                        s = t16[8 + q:9 + q]
                        k = t16[4 + q:5 + q]
                    else:
                        at = slice(T, D)
                        s = jnp.where(row16 < 4, pltpu.roll(t16, 8, 0), 0.0)
                        k = jnp.where(row16 < 4, pltpu.roll(t16, 12, 0), 0.0)
                    c = got[at, part] * s
                    if not (even and end):
                        S[h, idx, at, :] += c
                    cb = c.astype(BF16)
                    own, cor = block(z, 0).start, block(z, 3).start
                    B[h, own + at.start:own + at.stop, part] = (c * k).astype(BF16)
                    B[h, cor + at.start:cor + at.stop, part] = cb

        def neighbours(z):
            c = B[h, block(z, 3), :]
            t = c[T:]
            r16 = lax.broadcasted_iota(jnp.int32, (16, 2 * LANES), 0)
            xp = dot(jnp.concatenate([c[:2 * A], t], 0), XP[...])
            xm = dot(jnp.concatenate([c[2 * A:T], t], 0), XM[...])
            yp = dot(jnp.concatenate([c[:A], c[2 * A:3 * A], t], 0), YP[...])
            ym = dot(jnp.concatenate([c[A:2 * A], c[3 * A:T], t], 0), YM[...])
            o = block(z, 1).start
            B[h, o:o + 2 * A, :] = xp[:2 * A].astype(BF16)
            B[h, o + 2 * A:o + T, :] = xm[:2 * A].astype(BF16)
            B[h, o + T:o + D, :] = jnp.where(r16 < 2, xp[2 * A:], xm[2 * A:]).astype(BF16)
            o = block(z, 2).start
            B[h, o:o + A, :] = yp[:A].astype(BF16)
            B[h, o + A:o + 2 * A, :] = ym[:A].astype(BF16)
            B[h, o + 2 * A:o + 3 * A, :] = yp[A:2 * A].astype(BF16)
            B[h, o + 3 * A:o + T, :] = ym[A:2 * A].astype(BF16)
            B[h, o + T:o + D, :] = jnp.where(r16 % 2 == 0, yp[2 * A:], ym[2 * A:]).astype(BF16)

        def apply(z):
            acc = dot(W[z], B[h, 3 * z * D:(3 * z + 5) * D, :])
            for p in (0, 1):
                R[h, base + 2 * p + z] += acc[:, p * LANES:(p + 1) * LANES]

        solve(first)
        c_copy(h, base, t, low).start()
        solve(1 - first)
        if last is not None:
            @pl.when(last)
            def _():
                c2_copy(h, not low).start()
        neighbours(first)
        apply(first)
        end = base if low else base + L - 1

        rsb[h] = R[h, end].astype(BF16)
        if last is None:
            r_copy(h, base, t, low).start()
        else:
            pl.when(jnp.logical_not(last))(lambda: r_copy(h, base, t, low).start())
        neighbours(1 - first)
        apply(1 - first)
        if low:
            acc = z_down(B[h, block(1, 3), :])
            R[h, base + 2] += acc[:, :LANES]
            new, out = acc[:, LANES:], base + L
        else:
            acc = z_up(B[h, block(0, 3), :])
            R[h, base + 1] += acc[:, LANES:]
            new, out = acc[:, :LANES], base - 1
        R[h, out, :T, :] = new[:T]
        R[h, out, T:T + 4, :] = new[T:T + 4]

    def finish(h, base, t, even, last):
        low = base == 0
        out = base + L if low else base - 1
        c_copy(h, base, t, low).wait()
        c = cr[t, h]
        if low:
            acc = z_up(jnp.concatenate([B[h, block(0, 3), LANES:], c], 1))
            R[h, base + 1] += acc[:, :LANES]
            R[h, base + L - 1] += acc[:, LANES:]
        else:
            acc = z_down(jnp.concatenate([c, B[h, block(1, 3), :LANES]], 1))
            R[h, base] += acc[:, :LANES]
            R[h, base + 2] += acc[:, LANES:]
        if even:
            S[h, out] += c.astype(F32)

        def take():
            r_copy(h, base, t, low).wait()
            R[h, out, :T, :] += rr[t, h, :T, :].astype(F32)
            R[h, out, T:T + 4, :] += rr[t, h, T:, :].astype(F32)[:4]

        if last is None:
            take()
        else:
            pl.when(jnp.logical_not(last))(take)

            @pl.when(last)
            def _():
                c2_copy(h, not low).wait()
                other = base if low else base + L - 1
                R[h, other] += z_down(cr2[h]) if low else z_up(cr2[h])

    def between(h, u):
        def shift(d, down):
            for idx in range(L + 1):
                move(R, h, idx, d, down, idx == (L if h == 0 else 0))
            for z in range(L):
                move(S, h, z + 1 - h, d, down)

        @pl.when(lax.rem(u, 2) == 0)
        def _():
            shift(1, False)

        @pl.when(u == 1)
        def _():
            shift(0, False)
            shift(1, True)

    def out_copy(out, got, h, kind, o):
        s, where = in_plane(o)
        return remote(out.at[h, where["gx"] * ny + where["gy"]], got.at[h, slab],
                      64 + (2 * kind + h) * G + o, where)

    def send_out(ref, h, out, got, kind):
        for py in (0, 1):
            for r in range(0, A, 16):
                v = []
                for n in range(G):
                    first = (n % 2 * 2 + py) * A + r
                    v.append(ref[h, n // 2 + 1 - h, first:first + 16, :])
                for n, x in enumerate(swap_source(v)):
                    out[h, n, py * A + r:py * A + r + 16, :] = x.astype(BF16)
        v = []
        for n in range(G):
            t = ref[h, n // 2 + 1 - h, T:, :]
            v.append(pltpu.roll(t, 14, 0) if n % 2 else t)
        for n, x in enumerate(swap_source(v)):
            out[h, n, 2 * A:, :] = x.astype(BF16)
        for o in range(1, G):
            out_copy(out, got, h, kind, o).start()
        got[h, slab] = out[h, mine]

    def body(u, carry):
        begin(0, 0, 2 * u, True, None)

        @pl.when(u > 0)
        def _():
            finish(1, 0, 2 * u - 1, False, None)
            between(1, u - 1)

        pl.when(u == 0)(lambda: settle(1))
        begin(1, 1, 2 * u, True, None)
        finish(0, 0, 2 * u, True, None)
        begin(0, 1, 2 * u + 1, False, u == 3)
        pl.when(u == 3)(lambda: send_out(S, 0, osol, rsol, 0))
        finish(1, 1, 2 * u, True, None)
        begin(1, 0, 2 * u + 1, False, u == 3)
        pl.when(u == 3)(lambda: send_out(S, 1, osol, rsol, 0))
        finish(0, 1, 2 * u + 1, False, u == 3)
        pl.when(u == 3)(lambda: send_out(R, 0, ores, rres, 1))

        @pl.when(u < 3)
        def _():
            between(0, u)
        return carry

    lax.fori_loop(0, 4, body, 0)

    finish(1, 0, 7, False, jnp.bool_(True))
    send_out(R, 1, ores, rres, 1)

    def unpack(got, out):
        def merge(at):
            pairs = [swap([got[0, s, at, :].astype(F32), got[1, s, at, :].astype(F32)], 1, 2)
                     for s in range(G)]
            return [swap_slab([p[px] for p in pairs]) for px in (0, 1)]

        for py in (0, 1):
            for r in range(0, A, 16):
                v = merge(slice(py * A + r, py * A + r + 16))
                for px in (0, 1):
                    for (i, j), x in zip(cells, v[px]):
                        out[2 * i + px, 2 * j + py, r:r + 16, :] = x
        v = merge(slice(2 * A, M))
        for px in (0, 1):
            for (i, j), x in zip(cells, v[px]):
                for py in (0, 1):
                    out[2 * i + px, 2 * j + py, A:A + 1, :] = x[py:py + 1]

    for h in (0, 1):
        for o in range(1, G):
            out_copy(osol, rsol, h, 0, o).wait()
    unpack(rsol, sol_ref)
    for h in (0, 1):
        for o in range(1, G):
            out_copy(ores, rres, h, 1, o).wait()
    unpack(rres, res_ref)


def in_slabs(sizes, right_side, cell_coef, cell_matrix, face_coupling, patch_inverse):
    Q = cell_matrix.shape[0]
    X, Y, Z = cell_coef.shape
    lanes = right_side.shape[3]
    nx, ny, nz = sizes
    G = nx * ny
    D = 4 * (Q - 1) + 16
    coef = cell_coef.reshape(X * Y, Z)
    V = pltpu.VMEM
    half = (D, LANES)
    side = (2 * LANES, 2 * LANES)
    block = (X, Y, Q, lanes)
    piece = (2, G, 2 * (Q - 1) + 16, LANES)
    scratch = [
        V((X * Y, lanes), F32), V((X * Y, lanes), F32),
        V(piece, BF16), V(piece, BF16),
        V((2, 5, *half), F32), V((2, 5, *half), F32),
        V((2, 2 * D, 2 * LANES), BF16), V((2, 8 * D, 2 * LANES), BF16),
        V((2, D, 5 * D), BF16), V((2 * D, 2 * D), BF16),
        V(side, BF16), V(side, BF16), V(side, BF16), V(side, BF16),
        V((D, 4 * LANES), F32), V((2 * D, 8 * Q), BF16),
        V((8, 2, *half), BF16), V((8, 2, *half), BF16), V((2, *half), BF16), V((2, *half), BF16),
        V(piece, BF16), V(piece, BF16), V(piece, BF16), V(piece, BF16),
        pltpu.SemaphoreType.DMA((96,)), pltpu.SemaphoreType.DMA((96,)),
    ]
    vmem = pl.BlockSpec(memory_space=pltpu.VMEM)
    sol, res = pl.pallas_call(
        functools.partial(slab_kernel, sizes, (Q, nx, ny, nz, X // 2, Y // 2)),
        out_shape=[jax.ShapeDtypeStruct(block, F32)] * 2,
        in_specs=[vmem] * 5,
        out_specs=[vmem] * 2,
        scratch_shapes=scratch,
        compiler_params=pltpu.CompilerParams(
            collective_id=0, has_side_effects=True, vmem_limit_bytes=46 * 1024 * 1024),
    )(jnp.transpose(right_side, (1, 2, 0, 3)), coef, patch_inverse, cell_matrix, face_coupling)
    return tuple(jnp.transpose(x, (2, 0, 1, 3)) for x in (sol, res))


def on_device(sizes, right_side, cell_coef, cell_matrix, face_coupling, patch_inverse):
    X, Y, Z = cell_coef.shape
    form = in_slabs if fits_slabs(sizes, cell_matrix.shape[0], X, Y, Z, right_side.shape[3]) else in_blocks
    return form(sizes, right_side, cell_coef, cell_matrix, face_coupling, patch_inverse)


def solution(mesh):
    sizes = tuple(mesh.shape[a] for a in AXES)
    placed = (P(None, "gx", "gy", "gz"), P("gx", "gy", "gz"), P(), P(), P())
    return jax.shard_map(
        functools.partial(on_device, sizes),
        mesh=mesh,
        in_specs=placed,
        out_specs=(P(None, "gx", "gy", "gz"), P(None, "gx", "gy", "gz")),
        check_vma=False,
    )
```

```python
import functools
import jax
import jax.numpy as jnp
from jax import lax
from jax.experimental import pallas as pl
from jax.experimental.pallas import tpu as pltpu
from jax.sharding import PartitionSpec as P

AXES = ("gx", "gy", "gz")
MESH = pl.DeviceIdType.MESH
F32, BF16 = jnp.float32, jnp.bfloat16
LANES = 128


def class_pairs(d):
    bit = 4 >> d
    return [(c, c + bit) for c in range(8) if not c & bit]


def block_kernel(sizes, dims, start_ref, inverse_ref, w_ref, sol_ref, res_ref,
           R, S2, Sx, scaled, corr, ccorr, Xx, Xy, Xz,
           fx, fxe, fy, fz, fxes, fys, fzs, mxr, mxe, mxs, myr, mys, mzr,
           mxr_s, mxs_s, myr_s, mys_s, mzr_s, p_rows, p_ref, send_sem, recv_sem):
    D, Q, nr, ni, njh = dims
    w = 2 * nr
    A = Q // 16 * 16
    tiles = [(i, jh) for i in range(ni) for jh in range(njh)]
    C = ni * njh * LANES
    half = njh * LANES
    lane = lax.broadcasted_iota(jnp.int32, (D, LANES), 1)
    jlo0 = (lane // nr) % 2 == 0
    piece = lane // w

    me = [lax.axis_index(a) for a in AXES]

    def neighbour(d, step):
        n = sizes[d]
        return {AXES[d]: lax.rem(me[d] + step + n, n)}

    barrier = pltpu.get_barrier_semaphore()
    for d in range(3):
        for step in (1, -1):
            pl.semaphore_signal(barrier, inc=1, device_id=neighbour(d, step), device_id_type=MESH)

    def rows(c):
        return slice(c * D, (c + 1) * D)

    def cols(i, jh):
        t = i * njh + jh
        return slice(t * LANES, (t + 1) * LANES)

    def get(ref, c):
        return {t: ref[c, :, cols(*t)].astype(F32) for t in tiles}

    def roll(x, s):
        s = s % LANES
        return pltpu.roll(x, s, 1) if s else x

    for c in range(0, 8, 2):
        ox, oy = c // 4, c // 2 % 2
        for i, jh in tiles:
            a = start_ref[2 * i + ox, 4 * jh + oy]
            b = start_ref[2 * i + ox, 4 * jh + 2 + oy]
            R[c, :, cols(i, jh)] = jnp.where(jlo0, a, roll(b, nr))
            R[c + 1, :, cols(i, jh)] = jnp.where(jlo0, roll(a, -nr), b)
    S2[...] = jnp.zeros_like(S2)
    pl.semaphore_wait(barrier, 6)

    def pack_y(ref, last):
        out = []
        for p in class_pairs(1):
            c = p[1] if last else p[0]
            jh = njh - 1 if last else 0
            t0 = ref[c, :, cols(0, jh)].astype(F32)
            t1 = ref[c, :, cols(1, jh)].astype(F32)
            if last:
                out.append(jnp.where(jlo0, roll(t1, -nr), t0))
            else:
                out.append(jnp.where(jlo0, t0, roll(t1, nr)))
        return jnp.stack(out, 0)

    def pack_z(ref, last):
        acc = jnp.zeros((D, LANES), F32)
        n = 0
        for p in class_pairs(2):
            c = p[1] if last else p[0]
            for t in tiles:
                x = ref[c, :, cols(*t)].astype(F32)
                x = roll(x, w * (n + 1) if last else w * n)
                acc = jnp.where(piece == n, x, acc)
                n += 1
        return acc

    def shifted(d, step, have, halo, pc):
        out = {}
        for i, jh in tiles:
            if d == 0:
                at = i + step
                if 0 <= at < ni:
                    new = have[at, jh]
                else:
                    new = halo(slice(jh * LANES, (jh + 1) * LANES))
            elif d == 1:
                at = jh + step
                if 0 <= at < njh:
                    other = roll(have[i, at], step * nr)
                else:
                    other = halo(slice(0, LANES))
                    if i == 0:
                        other = roll(other, step * nr)
                cur = roll(have[i, jh], -step * nr)
                new = jnp.where(jlo0, cur, other) if step == 1 else jnp.where(jlo0, other, cur)
            else:
                n = pc * len(tiles) + i * njh + jh
                h = halo(slice(0, LANES))
                if step == 1:
                    new = jnp.where(lane >= LANES - w, roll(h, LANES - w - w * n),
                                    roll(have[i, jh], -w))
                else:
                    new = jnp.where(lane < w, roll(h, -w * n), roll(have[i, jh], w))
            out[i, jh] = new
        return out

    def read_x(t, last, pc):
        first = lax.broadcasted_iota(jnp.int32, (D - A, LANES), 0) == 0

        def halo(c):
            tail = fxe[t, last, :, c].astype(F32)[pc:pc + 1]
            return jnp.concatenate(
                [fx[t, last, pc, :, c].astype(F32), jnp.where(first, tail, 0.0)], 0)
        return halo

    def read_y(ref, *at):
        return lambda c: ref[(*at, slice(None), c)].astype(F32)

    def remote(src, dst, k, d, step):
        return pltpu.make_async_remote_copy(
            src_ref=src, dst_ref=dst, send_sem=send_sem.at[k], recv_sem=recv_sem.at[k],
            device_id=neighbour(d, step), device_id_type=MESH)

    def move(d, down, copies, halo, beside=None):
        for copy in copies:
            copy.start()
        if beside is not None:
            beside()
        for copy in copies:
            copy.wait()
        for pc, (c0, c1) in enumerate(class_pairs(d)):
            old0, old1 = get(R, c0), get(R, c1)
            if down:
                new0, new1 = shifted(d, -1, old1, halo(pc), pc), old0
            else:
                new0, new1 = old1, shifted(d, 1, old0, halo(pc), pc)
            for t in tiles:
                R[c0, :, cols(*t)] = new0[t]
                R[c1, :, cols(*t)] = new1[t]

    def move_x(down, at, beside=None):
        part = slice((ni - 1) * half, ni * half) if down else slice(0, half)
        cs = slice(4, 8) if down else slice(0, 4)
        mxr_s[...] = R[cs, :A, part].astype(BF16)
        step = 1 if down else -1
        copies = [remote(mxr_s, mxr.at[at], 72 + at, 0, step),
                  remote(R.at[cs, A:A + 8, part], mxe.at[at], 74 + at, 0, step)]
        zeros = jnp.zeros((D - A - 8, LANES), F32)

        def halo(pc):
            return lambda c: jnp.concatenate(
                [mxr[at, pc, :, c].astype(F32), mxe[at, pc, :, c], zeros], 0)
        move(0, down, copies, halo, beside)

    def move_y(down, u):
        myr_s[...] = pack_y(R, down)
        move(1, down, [remote(myr_s, myr.at[u], 64 + u, 1, 1 if down else -1)],
             lambda pc: read_y(myr, u, pc))

    def move_z(down, t):
        mzr_s[...] = pack_z(R, down)
        move(2, down, [remote(mzr_s, mzr.at[t], 48 + t, 2, 1 if down else -1)],
             lambda pc: read_y(mzr, t))

    def sol_y(u):
        return remote(mys_s, mys.at[lax.div(u, 2)], 56 + lax.div(u, 2), 1, -1)

    def sol_x():
        return remote(mxs_s, mxs, 58, 0, -1)

    def pair(ref, q):
        return ref[2 * q:2 * q + 2].reshape(2 * D, C)

    def lessen(q, acc):
        R[2 * q:2 * q + 2] -= acc.reshape(2, D, C)

    def dot(a, b):
        return jnp.dot(a, b, preferred_element_type=F32)

    def colour(t, v, sb):
        for c in range(8):
            s = R[c, Q:Q + 1, :]
            scaled[c] = (s * R[c]).astype(BF16)
        copies = [[None, None] for _ in range(3)]
        extra = [None, None]
        line = lax.broadcasted_iota(jnp.int32, (16, half), 0)
        for n in range(ni):
            part = slice(n * half, (n + 1) * half)
            solved = dot(p_ref[...], scaled[:, :, part].reshape(8 * D, half))
            for c in range(8):
                s = R[c, Q:Q + 1, part]
                k = R[c, Q + 1:Q + 2, part]
                got = s * solved[rows(c), :]
                if v == 1:
                    S2[sb, c, :, part] += got
                corr[c, :, part] = got.astype(BF16)
                ccorr[c, :, part] = (k * got).astype(BF16)
            for last in (0, 1):
                if n != (ni - 1 if last else 0):
                    continue
                step = 1 if last else -1
                tail = jnp.zeros((16, half), F32)
                for pc in range(4):
                    row = corr[4 * last + pc, A:, part].astype(F32)[:1]
                    tail = jnp.where(line == pc, row, tail)
                fxes[last] = tail.astype(BF16)
                copies[0][last] = remote(corr.at[4 * last:4 * last + 4, :A, part], fx.at[t, last],
                                         t * 6 + last, 0, step)
                copies[0][last].start()
                extra[last] = remote(fxes.at[last], fxe.at[t, last], 80 + 2 * t + last, 0, step)
                extra[last].start()
        for last in (0, 1):
            fzs[last] = pack_z(corr, last).astype(BF16)
            copies[2][last] = remote(fzs.at[last], fz.at[t, last], t * 6 + 4 + last, 2, 1 if last else -1)
            copies[2][last].start()
        for last in (0, 1):
            fys[last] = pack_y(corr, last).astype(BF16)
            copies[1][last] = remote(fys.at[last], fy.at[t, last], t * 6 + 2 + last, 1, 1 if last else -1)
            copies[1][last].start()
        for q in range(4):
            acc = dot(w_ref[0], pair(ccorr, q))
            acc += dot(w_ref[1], pair(corr, q))
            acc += dot(w_ref[3 if q // 2 == 0 else 4], pair(corr, q ^ 2))
            acc += dot(w_ref[5 if q % 2 == 0 else 6], pair(corr, q ^ 1))
            lessen(q, acc)

        def fill(d, X, halo0, halo1):
            for pc, (c0, c1) in enumerate(class_pairs(d)):
                new0 = shifted(d, 1, get(corr, c0), halo0(pc), pc)
                new1 = shifted(d, -1, get(corr, c1), halo1(pc), pc)
                for at in tiles:
                    X[c0, :, cols(*at)] = new0[at].astype(BF16)
                    X[c1, :, cols(*at)] = new1[at].astype(BF16)

        for copy in copies[2]:
            copy.wait()
        fill(2, Xz, lambda pc: read_y(fz, t, 0), lambda pc: read_y(fz, t, 1))
        if v == 0:
            for c0, c1 in class_pairs(2):
                S2[sb, c0] += corr[c1].astype(F32)
                S2[sb, c1] += Xz[c0].astype(F32)
        for copy in copies[1]:
            copy.wait()
        fill(1, Xy, lambda pc: read_y(fy, t, 0, pc), lambda pc: read_y(fy, t, 1, pc))
        for q in range(4):
            acc = dot(w_ref[2], pair(Xz, q))
            acc += dot(w_ref[6 if q % 2 == 0 else 5], pair(Xy, q ^ 1))
            lessen(q, acc)
        for copy in copies[0] + extra:
            copy.wait()
        fill(0, Xx, lambda pc: read_x(t, 0, pc), lambda pc: read_x(t, 1, pc))
        for q in range(4):
            lessen(q, dot(w_ref[4 if q // 2 == 0 else 3], pair(Xx, q ^ 2)))

    def class_order():
        r = lax.broadcasted_iota(jnp.int32, (D, 8 * Q), 0)
        k = lax.broadcasted_iota(jnp.int32, (D, 8 * Q), 1)
        for c in range(8):
            pick = jnp.where((k == r * 8 + c) & (r < Q), 1.0, 0.0).astype(BF16)
            p_rows[c * D:(c + 1) * D, :] = dot(pick, inverse_ref[...]).astype(BF16)
        k = lax.broadcasted_iota(jnp.int32, (8 * Q, 8 * D), 0)
        r = lax.broadcasted_iota(jnp.int32, (8 * Q, 8 * D), 1)
        q = r % D
        pick = jnp.where((k == q * 8 + r // D) & (q < Q), 1.0, 0.0).astype(BF16)
        p_ref[...] = dot(p_rows[...], pick).astype(BF16)

    def body(u, carry):
        @pl.when(u == 0)
        def _():
            move_x(True, 0, class_order)

        @pl.when(u == 2)
        def _():
            move_x(False, 1)
            for c in range(8):
                Sx[c] = S2[1, c]
            mxs_s[...] = S2[1, :4, :, :half].astype(BF16)
            sol_x().start()
            S2[1] = jnp.zeros_like(Sx)

        @pl.when(lax.rem(u, 2) == 0)
        def _():
            S2[0] = jnp.zeros_like(Sx)
            move_y(True, u)

        @pl.when(lax.rem(u, 2) == 1)
        def _():
            move_y(False, u)
            mys_s[...] = pack_y(S2.at[0], False).astype(BF16)
            sol_y(u).start()

        for v in (0, 1):
            t = 2 * u + v
            move_z(v == 0, t)
            colour(t, v, lax.rem(u, 2))

        @pl.when(lax.rem(u, 2) == 1)
        def _():
            sol_y(u).wait()
            for pc, (c0, c1) in enumerate(class_pairs(1)):
                S2[1, c0] += S2[0, c1]
                new = shifted(1, 1, get(S2.at[0], c0), read_y(mys, lax.div(u, 2), pc), pc)
                for at in tiles:
                    S2[1, c1, :, cols(*at)] += new[at]
        return carry

    lax.fori_loop(0, 4, body, 0)
    sol_x().wait()
    for pc, (c0, c1) in enumerate(class_pairs(0)):
        S2[1, c0] += Sx[c1]
        new = shifted(0, 1, get(Sx, c0), read_y(mxs, pc), pc)
        for at in tiles:
            S2[1, c1, :, cols(*at)] += new[at]

    for ref, out in ((S2.at[1], sol_ref), (R, res_ref)):
        for c in range(0, 8, 2):
            ox, oy = c // 4, c // 2 % 2
            for i, jh in tiles:
                x0 = ref[c, :, cols(i, jh)]
                x1 = ref[c + 1, :, cols(i, jh)]
                out[2 * i + ox, 4 * jh + oy] = jnp.where(jlo0, x0, roll(x1, nr))
                out[2 * i + ox, 4 * jh + 2 + oy] = jnp.where(jlo0, roll(x0, -nr), x1)


def in_blocks(sizes, right_side, cell_coef, cell_matrix, face_coupling, patch_inverse):
    Q = cell_matrix.shape[0]
    X, Y, Z = cell_coef.shape
    lanes = right_side.shape[3]
    nr = lanes // Z
    D = -(-(Q + 2) // 16) * 16
    ni, njh = X // 2, Y // 4
    assert lanes == LANES and ni == 2 and 4 * ni * njh * 2 * nr == LANES
    C = ni * njh * LANES
    coef = jnp.repeat(cell_coef, nr, axis=2)
    extra = jnp.stack([lax.rsqrt(coef), coef], 2)
    start = jnp.concatenate(
        [jnp.transpose(right_side, (1, 2, 0, 3)), extra, jnp.zeros((X, Y, D - Q - 2, lanes), F32)], 2)
    def padded(m):
        return jnp.pad(m, ((0, D - Q), (0, D - Q)))

    zero = jnp.zeros((D, D), F32)

    def both(a, b, c, d):
        return jnp.concatenate([jnp.concatenate([a, b], 1), jnp.concatenate([c, d], 1)], 0)

    m = padded(cell_matrix)
    f = [-padded(face_coupling[d]) for d in range(3)]
    ft = [x.T for x in f]
    mats = jnp.stack([
        both(m, zero, zero, m),
        both(zero, f[2], ft[2], zero),
        both(zero, ft[2], f[2], zero),
        both(f[0], zero, zero, f[0]),
        both(ft[0], zero, zero, ft[0]),
        both(f[1], zero, zero, f[1]),
        both(ft[1], zero, zero, ft[1]),
    ]).astype(BF16)
    half = njh * LANES
    V = pltpu.VMEM
    A = Q // 16 * 16
    assert Q == A + 1
    whole = (8, D, C)
    scratch = [
        V(whole, F32), V((2, *whole), F32), V(whole, F32), V(whole, BF16), V(whole, BF16), V(whole, BF16),
        V(whole, BF16), V(whole, BF16), V(whole, BF16),
        V((8, 2, 4, A, half), BF16), V((8, 2, 16, half), BF16),
        V((8, 2, 4, D, LANES), BF16), V((8, 2, D, LANES), BF16),
        V((2, 16, half), BF16), V((2, 4, D, LANES), BF16), V((2, D, LANES), BF16),
        V((2, 4, A, half), BF16), V((2, 4, 8, half), F32), V((4, D, half), BF16),
        V((4, 4, D, LANES), F32), V((2, 4, D, LANES), BF16), V((8, D, LANES), F32),
        V((4, A, half), BF16), V((4, D, half), BF16),
        V((4, D, LANES), F32), V((4, D, LANES), BF16), V((D, LANES), F32),
        V((8 * D, 8 * Q), BF16), V((8 * D, 8 * D), BF16),
        pltpu.SemaphoreType.DMA((96,)), pltpu.SemaphoreType.DMA((96,)),
    ]
    vmem = pl.BlockSpec(memory_space=pltpu.VMEM)
    sol, res = pl.pallas_call(
        functools.partial(block_kernel, sizes, (D, Q, nr, ni, njh)),
        out_shape=[jax.ShapeDtypeStruct((X, Y, D, lanes), F32)] * 2,
        in_specs=[vmem] * 3,
        out_specs=[vmem] * 2,
        scratch_shapes=scratch,
        compiler_params=pltpu.CompilerParams(
            collective_id=0, has_side_effects=True, vmem_limit_bytes=46 * 1024 * 1024),
    )(start, patch_inverse, mats)
    return tuple(jnp.transpose(x[:, :, :Q], (2, 0, 1, 3)) for x in (sol, res))


def fits_slabs(sizes, Q, X, Y, Z, lanes):
    group = sizes[0] * sizes[1]
    layers = Z // group
    return (lanes == LANES and Q % 16 == 1 and layers == 4 and Z == layers * group
            and (X // 2) * (Y // 2) == group and lanes // Z == 4 and 2 * layers == group
            and X % 2 == 0 and Y % 2 == 0)


def slab_kernel(sizes, dims, start_ref, coef_ref, inverse_ref, m_ref, f_ref, sol_ref, res_ref,
                coef_high, coef_low, msg, rx, R, S, X, B, W, P, XP, XM, YP, YM, U, p_rows,
                cr, rr, cr2, rsb, osol, ores, rsol, rres, send_sem, recv_sem):
    Q, nx, ny, nz, hx, hy = dims
    G = nx * ny
    L = 4
    A = Q - 1
    T = 4 * A
    D = T + 16
    wide = 1
    while wide * wide < nx:
        wide += 1
    lane = lax.broadcasted_iota(jnp.int32, (1, LANES), 1)
    row16 = lax.broadcasted_iota(jnp.int32, (16, LANES), 0)

    gx, gy, gz = [lax.axis_index(a) for a in AXES]
    mine = gx * ny + gy

    def snake(p):
        row = p // wide
        col = p % wide
        return row * wide + col + (row % 2) * (wide - 1 - 2 * col)

    def flip(p, plane):
        return p + (plane % 2) * (nx - 1 - 2 * p)

    slab = flip(snake(gx), gz) * ny + gy

    def device(plane, s):
        return {"gx": snake(flip(s // ny, plane)), "gy": s % ny, "gz": plane}

    def ring(step):
        g = lax.rem(gz * G + slab + step + nz * G, nz * G)
        return device(g // G, g % G)

    def in_plane(o):
        s = lax.rem(slab + o, G)
        return s, device(gz, s)

    barrier = pltpu.get_barrier_semaphore()
    for o in range(1, G):
        pl.semaphore_signal(barrier, inc=1, device_id=in_plane(o)[1], device_id_type=MESH)
    for step in (1, -1):
        pl.semaphore_signal(barrier, inc=1, device_id=ring(step), device_id_type=MESH)

    def remote(src, dst, k, where):
        return pltpu.make_async_remote_copy(
            src_ref=src, dst_ref=dst, send_sem=send_sem.at[k], recv_sem=recv_sem.at[k],
            device_id=where, device_id_type=MESH)

    def roll(x, s):
        s = s % LANES
        return pltpu.roll(x, s, 1) if s else x

    def swap(v, index_bit, weight):
        out = list(v)
        low = (lane // weight) % 2 == 0
        for n in range(len(v)):
            if n & index_bit:
                continue
            a, b = v[n], v[n | index_bit]
            out[n] = jnp.where(low, a, roll(b, weight))
            out[n | index_bit] = jnp.where(low, roll(a, -weight), b)
        return out

    bits = [1 << b for b in range(G.bit_length() - 1)]
    WS = 4 * L

    def swap_slab(v):
        for b in bits:
            v = swap(v, b, WS * b)
        return v

    def swap_source(v):
        for b in bits:
            v = swap(v, b, 2 * b)
        return v

    def lane_x(l):
        return (l // (2 * ny)) % nx * hx + (l // (WS * hy)) % hx

    def lane_y(l):
        return (l // 2) % ny * hy + (l // WS) % hy

    def shift_x(v, step):
        assert hx == 2
        i0 = (lane // (WS * hy)) % 2
        g = (lane // (2 * ny)) % nx
        half, one, all_ = WS * hy, 2 * ny, 2 * ny * (nx - 1)
        flat = roll(v, half)
        if step == 1:
            carry = jnp.where(g < nx - 1, roll(v, half - one), roll(v, half + all_))
            return jnp.where(i0 == 0, flat, carry)
        carry = jnp.where(g > 0, roll(v, half + one), roll(v, half - all_))
        return jnp.where(i0 == 1, flat, carry)

    def shift_y(v, step):
        assert ny == 2
        j0 = (lane // WS) % hy
        g = (lane // 2) % 2
        back = WS * (hy - 1)
        if step == 1:
            carry = jnp.where(g == 0, roll(v, back - 2), roll(v, back + 2))
            return jnp.where(j0 < hy - 1, roll(v, -WS), carry)
        carry = jnp.where(g == 0, roll(v, -back - 2), roll(v, -back + 2))
        return jnp.where(j0 > 0, roll(v, WS), carry)

    def class_rows(q):
        return slice(q * A, (q + 1) * A)

    cells = [(i, j) for i in range(hx) for j in range(hy)]
    M = 2 * A + 16

    def tail_tile(px, i, j):
        out = jnp.zeros((16, LANES), F32)
        for py in (0, 1):
            x, y = 2 * i + px, 2 * j + py
            at = slice(2 * hy * x + y, 2 * hy * x + y + 1)
            out = jnp.where(row16 == py, start_ref[x, y, A:A + 1, :], out)
            out = jnp.where(row16 == 4 + py, coef_high[at, :], out)
            out = jnp.where(row16 == 8 + py, coef_low[at, :], out)
        return out

    zs = coef_ref.shape[1]
    spread = (lax.broadcasted_iota(jnp.int32, (zs, LANES), 1) // (LANES // zs)
              == lax.broadcasted_iota(jnp.int32, (zs, LANES), 0))
    spread = jnp.where(spread, 1.0, 0.0).astype(BF16)
    high = coef_ref[...].astype(BF16)
    low = (coef_ref[...] - high.astype(F32)).astype(BF16)
    coef_high[...] = jnp.dot(high, spread, preferred_element_type=F32)
    coef_low[...] = jnp.dot(low, spread, preferred_element_type=F32)

    def pack(tiles, at):
        v = [swap_slab(t) for t in tiles]
        for s in range(G):
            for half, x in enumerate(swap([v[0][s], v[1][s]], 1, 2)):
                msg[half, s, at, :] = x.astype(BF16)

    for py in (0, 1):
        for r in range(0, A, 16):
            pack([[start_ref[2 * i + px, 2 * j + py, r:r + 16, :] for i, j in cells] for px in (0, 1)],
                 slice(py * A + r, py * A + r + 16))
    pack([[tail_tile(px, i, j) for i, j in cells] for px in (0, 1)], slice(2 * A, M))
    pl.semaphore_wait(barrier, G + 1)
    arrivals = []
    for half in (0, 1):
        arrivals.append([])
        for o in range(1, G):
            s, where = in_plane(o)
            arrivals[half].append(
                remote(msg.at[half, s], rx.at[half, mine], 32 + G * half + o, where))
            arrivals[half][-1].start()
    for half in (0, 1):
        rx[half, mine] = msg[half, slab]

    def dot(a, b):
        return jnp.dot(a, b, preferred_element_type=F32)

    def dot_t(a, b):
        return lax.dot_general(a, b, (((1,), (1,)), ((), ())), preferred_element_type=F32)

    def iota(shape, d):
        return lax.broadcasted_iota(jnp.int32, shape, d)

    def one_hot(hit):
        return jnp.where(hit, 1.0, 0.0).astype(BF16)

    wide2 = 2 * LANES
    src, dst = iota((wide2, 1), 0), iota((1, wide2), 1)

    def column(l, x_step, y_step):
        n = l % LANES
        x, y = (lane_x(n) + x_step) % (hx * nx), (lane_y(n) + y_step) % (hy * ny)
        return ((l // LANES * 2 + l % 2) * (hx * nx) + x) * (hy * ny) + y

    for ref, x_step, y_step in ((XP, 1, 0), (XM, hx * nx - 1, 0), (YP, 0, 1), (YM, 0, hy * ny - 1)):
        ref[...] = one_hot(column(src, 0, 0) == column(dst, x_step, y_step))

    def patch_row(k):
        d, c = k // 8, k % 8
        return c % 2 * D + jnp.where(d < A, c // 2 * A + d, T + c // 2)

    pick = one_hot(patch_row(iota((1, 8 * Q), 1)) == iota((2 * D, 8 * Q), 0))
    p_rows[...] = dot(pick, inverse_ref[...]).astype(BF16)
    pick = one_hot(patch_row(iota((8 * Q, 1), 0)) == iota((8 * Q, 2 * D), 1))
    P[...] = dot(p_rows[...], pick).astype(BF16)

    def packed(k):
        q, d = k // LANES, k % LANES
        return jnp.where(d < A, q * A + d, jnp.where(d == A, T + q, -1))

    cols = one_hot(packed(iota((4 * LANES, 1), 0)) == iota((4 * LANES, D), 1))
    eye = one_hot(iota((D, 1), 0) == iota((D, D), 1))

    def table(blocks):
        U[...] = jnp.zeros_like(U)
        for a, b, m in blocks:
            U[a * A:(a + 1) * A, b * LANES:b * LANES + Q] = m[:A]
            U[T + a:T + a + 1, b * LANES:b * LANES + Q] = m[A:]
        return dot(U[...].astype(BF16), cols).astype(BF16)

    def turned(w):
        return dot_t(eye, w).astype(BF16)

    fx, fy, fz = f_ref[0], f_ref[1], f_ref[2]
    order = ((0, 1, 2, 3, 4), (2, 3, 4, 1, 0))

    def put(k, w):
        for z in (0, 1):
            W[z, :, order[z][k] * D:(order[z][k] + 1) * D] = w[z]

    w = table([(q, q, -m_ref[...]) for q in range(4)])
    put(0, (w, w))
    w = table([(2, 0, fx), (3, 1, fx)])
    w += turned(w)
    put(1, (w, w))
    w = table([(1, 0, fy), (3, 2, fy)])
    w += turned(w)
    put(2, (w, w))
    w = table([(0, 2, fx), (1, 3, fx), (0, 1, fy), (2, 3, fy)])
    w += turned(w)
    put(3, (w, w))
    w = table([(q, q, fz) for q in range(4)])
    put(4, (w, turned(w)))
    S[...] = jnp.zeros_like(S)

    def z_up(c):
        return dot(W[0, :, 4 * D:], c)

    def z_down(c):
        return dot(W[1, :, :D], c)

    def arrive(h):
        for copy in arrivals[h]:
            copy.wait()
        for py in (0, 1):
            for r in range(0, A, 16):
                at = slice(py * A + r, py * A + r + 16)
                v = swap_source([rx[h, n, at, :].astype(F32) for n in range(G)])
                for n in range(G):
                    first = (n % 2 * 2 + py) * A + r
                    R[h, n // 2 + 1 - h, first:first + 16, :] = v[n]
        v = swap_source([rx[h, n, 2 * A:, :].astype(F32) for n in range(G)])
        for z in range(L):
            R[h, z + 1 - h, T:, :] = jnp.where(row16 % 4 < 2, v[2 * z], pltpu.roll(v[2 * z + 1], 2, 0))

    def move(ref, h, idx, d, down, only_tail=False):
        shift = shift_x if d == 0 else shift_y
        bit = 2 >> d
        for q in range(4):
            if q & bit or only_tail:
                continue
            old0 = ref[h, idx, class_rows(q), :]
            old1 = ref[h, idx, class_rows(q + bit), :]
            if down:
                ref[h, idx, class_rows(q), :] = shift(old1, -1)
                ref[h, idx, class_rows(q + bit), :] = old0
            else:
                ref[h, idx, class_rows(q), :] = old1
                ref[h, idx, class_rows(q + bit), :] = shift(old0, 1)
        t = ref[h, idx, T:, :]
        upper = (row16 // bit) % 2 == 1
        if down:
            t = jnp.where(upper, shift(t, -1), t)
        else:
            t = jnp.where(upper, t, shift(t, 1))
        ref[h, idx, T:, :] = jnp.where(upper, pltpu.roll(t, bit, 0), pltpu.roll(t, 16 - bit, 0))

    def first_copy(h):
        return remote(rsb.at[h], rr.at[7, h], 60 + h, ring(1 if h == 0 else -1))

    def enter(h):
        arrive(h)
        end = L if h == 0 else 0
        for idx in [end] + [z + 1 - h for z in range(L) if z + 1 - h != end]:
            for d in (0, 1):
                move(R, h, idx, d, True)
            if idx == end:
                rsb[h] = R[h, end].astype(BF16)
                first_copy(h).start()

    def settle(h):
        first_copy(h).wait()
        R[h, 0 if h == 0 else L] = rr[7, h].astype(F32)
        for idx in range(L + 1):
            t = R[h, idx, T:, :]
            k = t + pltpu.roll(t, 12, 0)
            k = jnp.where((row16 >= 4) & (row16 < 8), k, 1.0)
            s = pltpu.roll(lax.rsqrt(k), 4, 0)
            t = jnp.where(row16 < 4, t, jnp.where(row16 < 8, k, jnp.where(row16 < 12, s, 0.0)))
            R[h, idx, T:, :] = t

    enter(0)
    enter(1)
    settle(0)

    def split(k):
        return k % 2, slice(k // 2 * LANES, (k // 2 + 1) * LANES)

    def block(z, k):
        n = 3 * z + order[z][k]
        return slice(n * D, (n + 1) * D)

    def c_copy(h, base, t, low):
        z, part = split(0 if low else L - 1)
        return remote(B.at[h, block(z, 3), part], cr.at[t, h], t * 4 + h, ring(-1 if low else 1))

    def r_copy(h, base, t, low):
        return remote(rsb.at[h], rr.at[t, h], t * 4 + 2 + h, ring(-1 if low else 1))

    def c2_copy(h, low):
        z, part = split(0 if low else L - 1)
        return remote(B.at[h, block(z, 3), part], cr2.at[h], 62 + h, ring(-1 if low else 1))

    def begin(h, base, t, even, last):
        low = base == 0
        first = 0 if low else 1
        for k in range(L):
            z, part = split(k)
            for q in range(4):
                s = R[h, base + k, T + 8 + q:T + 9 + q, :]
                X[h, z * D + q * A:z * D + (q + 1) * A, part] = (
                    R[h, base + k, class_rows(q), :] * s).astype(BF16)
            t16 = R[h, base + k, T:, :]
            x16 = jnp.where(row16 < 4, t16 * pltpu.roll(t16, 8, 0), 0.0)
            X[h, z * D + T:(z + 1) * D, part] = x16.astype(BF16)

        def solve(z):
            got = dot(P[z * D:(z + 1) * D, :], X[h])
            for p in (0, 1):
                idx = base + 2 * p + z
                part = slice(p * LANES, (p + 1) * LANES)
                end = 2 * p + z == (0 if low else L - 1)
                t16 = R[h, idx, T:, :]
                for q in range(5):
                    if q < 4:
                        at = class_rows(q)
                        s = t16[8 + q:9 + q]
                        k = t16[4 + q:5 + q]
                    else:
                        at = slice(T, D)
                        s = jnp.where(row16 < 4, pltpu.roll(t16, 8, 0), 0.0)
                        k = jnp.where(row16 < 4, pltpu.roll(t16, 12, 0), 0.0)
                    c = got[at, part] * s
                    if not (even and end):
                        S[h, idx, at, :] += c
                    cb = c.astype(BF16)
                    own, cor = block(z, 0).start, block(z, 3).start
                    B[h, own + at.start:own + at.stop, part] = (c * k).astype(BF16)
                    B[h, cor + at.start:cor + at.stop, part] = cb

        def neighbours(z):
            c = B[h, block(z, 3), :]
            t = c[T:]
            r16 = lax.broadcasted_iota(jnp.int32, (16, 2 * LANES), 0)
            xp = dot(jnp.concatenate([c[:2 * A], t], 0), XP[...])
            xm = dot(jnp.concatenate([c[2 * A:T], t], 0), XM[...])
            yp = dot(jnp.concatenate([c[:A], c[2 * A:3 * A], t], 0), YP[...])
            ym = dot(jnp.concatenate([c[A:2 * A], c[3 * A:T], t], 0), YM[...])
            o = block(z, 1).start
            B[h, o:o + 2 * A, :] = xp[:2 * A].astype(BF16)
            B[h, o + 2 * A:o + T, :] = xm[:2 * A].astype(BF16)
            B[h, o + T:o + D, :] = jnp.where(r16 < 2, xp[2 * A:], xm[2 * A:]).astype(BF16)
            o = block(z, 2).start
            B[h, o:o + A, :] = yp[:A].astype(BF16)
            B[h, o + A:o + 2 * A, :] = ym[:A].astype(BF16)
            B[h, o + 2 * A:o + 3 * A, :] = yp[A:2 * A].astype(BF16)
            B[h, o + 3 * A:o + T, :] = ym[A:2 * A].astype(BF16)
            B[h, o + T:o + D, :] = jnp.where(r16 % 2 == 0, yp[2 * A:], ym[2 * A:]).astype(BF16)

        def apply(z):
            acc = dot(W[z], B[h, 3 * z * D:(3 * z + 5) * D, :])
            for p in (0, 1):
                R[h, base + 2 * p + z] += acc[:, p * LANES:(p + 1) * LANES]

        solve(first)
        c_copy(h, base, t, low).start()
        solve(1 - first)
        if last is not None:
            @pl.when(last)
            def _():
                c2_copy(h, not low).start()
        neighbours(first)
        apply(first)
        end = base if low else base + L - 1

        rsb[h] = R[h, end].astype(BF16)
        if last is None:
            r_copy(h, base, t, low).start()
        else:
            pl.when(jnp.logical_not(last))(lambda: r_copy(h, base, t, low).start())
        neighbours(1 - first)
        apply(1 - first)
        if low:
            acc = z_down(B[h, block(1, 3), :])
            R[h, base + 2] += acc[:, :LANES]
            new, out = acc[:, LANES:], base + L
        else:
            acc = z_up(B[h, block(0, 3), :])
            R[h, base + 1] += acc[:, LANES:]
            new, out = acc[:, :LANES], base - 1
        R[h, out, :T, :] = new[:T]
        R[h, out, T:T + 4, :] = new[T:T + 4]

    def finish(h, base, t, even, last):
        low = base == 0
        out = base + L if low else base - 1
        c_copy(h, base, t, low).wait()
        c = cr[t, h]
        if low:
            acc = z_up(jnp.concatenate([B[h, block(0, 3), LANES:], c], 1))
            R[h, base + 1] += acc[:, :LANES]
            R[h, base + L - 1] += acc[:, LANES:]
        else:
            acc = z_down(jnp.concatenate([c, B[h, block(1, 3), :LANES]], 1))
            R[h, base] += acc[:, :LANES]
            R[h, base + 2] += acc[:, LANES:]
        if even:
            S[h, out] += c.astype(F32)

        def take():
            r_copy(h, base, t, low).wait()
            R[h, out, :T, :] += rr[t, h, :T, :].astype(F32)
            R[h, out, T:T + 4, :] += rr[t, h, T:, :].astype(F32)[:4]

        if last is None:
            take()
        else:
            pl.when(jnp.logical_not(last))(take)

            @pl.when(last)
            def _():
                c2_copy(h, not low).wait()
                other = base if low else base + L - 1
                R[h, other] += z_down(cr2[h]) if low else z_up(cr2[h])

    def between(h, u):
        def shift(d, down):
            for idx in range(L + 1):
                move(R, h, idx, d, down, idx == (L if h == 0 else 0))
            for z in range(L):
                move(S, h, z + 1 - h, d, down)

        @pl.when(lax.rem(u, 2) == 0)
        def _():
            shift(1, False)

        @pl.when(u == 1)
        def _():
            shift(0, False)
            shift(1, True)

    def out_copy(out, got, h, kind, o):
        s, where = in_plane(o)
        return remote(out.at[h, where["gx"] * ny + where["gy"]], got.at[h, slab],
                      64 + (2 * kind + h) * G + o, where)

    def piece_copy(o, n):
        s, where = in_plane(o)
        at = slice(0, A) if n == 0 else slice(A, M)
        return remote(ores.at[1, where["gx"] * ny + where["gy"], at], rres.at[1, slab, at],
                      96 + n * G + o, where)

    def send_out(ref, h, out, got, kind):
        for py in (0, 1):
            for r in range(0, A, 16):
                v = []
                for n in range(G):
                    first = (n % 2 * 2 + py) * A + r
                    v.append(ref[h, n // 2 + 1 - h, first:first + 16, :])
                for n, x in enumerate(swap_source(v)):
                    out[h, n, py * A + r:py * A + r + 16, :] = x.astype(BF16)
            if kind == 1 and h == 1 and py == 0:
                for o in range(1, G):
                    piece_copy(o, 0).start()
        v = []
        for n in range(G):
            t = ref[h, n // 2 + 1 - h, T:, :]
            v.append(pltpu.roll(t, 14, 0) if n % 2 else t)
        for n, x in enumerate(swap_source(v)):
            out[h, n, 2 * A:, :] = x.astype(BF16)
        for o in range(1, G):
            if kind == 1 and h == 1:
                piece_copy(o, 1).start()
            else:
                out_copy(out, got, h, kind, o).start()
        got[h, slab] = out[h, mine]

    def body(u, carry):
        begin(0, 0, 2 * u, True, None)

        @pl.when(u > 0)
        def _():
            finish(1, 0, 2 * u - 1, False, None)
            between(1, u - 1)

        pl.when(u == 0)(lambda: settle(1))
        begin(1, 1, 2 * u, True, None)
        finish(0, 0, 2 * u, True, None)
        begin(0, 1, 2 * u + 1, False, u == 3)
        pl.when(u == 3)(lambda: send_out(S, 0, osol, rsol, 0))
        finish(1, 1, 2 * u, True, None)
        begin(1, 0, 2 * u + 1, False, u == 3)
        pl.when(u == 3)(lambda: send_out(S, 1, osol, rsol, 0))
        finish(0, 1, 2 * u + 1, False, u == 3)
        pl.when(u == 3)(lambda: send_out(R, 0, ores, rres, 1))

        @pl.when(u < 3)
        def _():
            between(0, u)
        return carry

    lax.fori_loop(0, 4, body, 0)

    finish(1, 0, 7, False, jnp.bool_(True))
    send_out(R, 1, ores, rres, 1)

    def unpack(got, out, parts=(0, 1)):
        def merge(at):
            pairs = [swap([got[0, s, at, :].astype(F32), got[1, s, at, :].astype(F32)], 1, 2)
                     for s in range(G)]
            return [swap_slab([p[px] for p in pairs]) for px in (0, 1)]

        for py in parts:
            for r in range(0, A, 16):
                v = merge(slice(py * A + r, py * A + r + 16))
                for px in (0, 1):
                    for (i, j), x in zip(cells, v[px]):
                        out[2 * i + px, 2 * j + py, r:r + 16, :] = x
        if 1 not in parts:
            return
        v = merge(slice(2 * A, M))
        for px in (0, 1):
            for (i, j), x in zip(cells, v[px]):
                for py in (0, 1):
                    out[2 * i + px, 2 * j + py, A:A + 1, :] = x[py:py + 1]

    for h in (0, 1):
        for o in range(1, G):
            out_copy(osol, rsol, h, 0, o).wait()
    unpack(rsol, sol_ref)
    for o in range(1, G):
        out_copy(ores, rres, 0, 1, o).wait()
    for n in (0, 1):
        for o in range(1, G):
            piece_copy(o, n).wait()
        unpack(rres, res_ref, (n,))


def in_slabs(sizes, right_side, cell_coef, cell_matrix, face_coupling, patch_inverse):
    Q = cell_matrix.shape[0]
    X, Y, Z = cell_coef.shape
    lanes = right_side.shape[3]
    nx, ny, nz = sizes
    G = nx * ny
    D = 4 * (Q - 1) + 16
    coef = cell_coef.reshape(X * Y, Z)
    V = pltpu.VMEM
    half = (D, LANES)
    side = (2 * LANES, 2 * LANES)
    block = (X, Y, Q, lanes)
    piece = (2, G, 2 * (Q - 1) + 16, LANES)
    scratch = [
        V((X * Y, lanes), F32), V((X * Y, lanes), F32),
        V(piece, BF16), V(piece, BF16),
        V((2, 5, *half), F32), V((2, 5, *half), F32),
        V((2, 2 * D, 2 * LANES), BF16), V((2, 8 * D, 2 * LANES), BF16),
        V((2, D, 5 * D), BF16), V((2 * D, 2 * D), BF16),
        V(side, BF16), V(side, BF16), V(side, BF16), V(side, BF16),
        V((D, 4 * LANES), F32), V((2 * D, 8 * Q), BF16),
        V((8, 2, *half), BF16), V((8, 2, *half), BF16), V((2, *half), BF16), V((2, *half), BF16),
        V(piece, BF16), V(piece, BF16), V(piece, BF16), V(piece, BF16),
        pltpu.SemaphoreType.DMA((112,)), pltpu.SemaphoreType.DMA((112,)),
    ]
    vmem = pl.BlockSpec(memory_space=pltpu.VMEM)
    sol, res = pl.pallas_call(
        functools.partial(slab_kernel, sizes, (Q, nx, ny, nz, X // 2, Y // 2)),
        out_shape=[jax.ShapeDtypeStruct(block, F32)] * 2,
        in_specs=[vmem] * 5,
        out_specs=[vmem] * 2,
        scratch_shapes=scratch,
        compiler_params=pltpu.CompilerParams(
            collective_id=0, has_side_effects=True, vmem_limit_bytes=46 * 1024 * 1024),
    )(jnp.transpose(right_side, (1, 2, 0, 3)), coef, patch_inverse, cell_matrix, face_coupling)
    return tuple(jnp.transpose(x, (2, 0, 1, 3)) for x in (sol, res))


def on_device(sizes, right_side, cell_coef, cell_matrix, face_coupling, patch_inverse):
    X, Y, Z = cell_coef.shape
    form = in_slabs if fits_slabs(sizes, cell_matrix.shape[0], X, Y, Z, right_side.shape[3]) else in_blocks
    return form(sizes, right_side, cell_coef, cell_matrix, face_coupling, patch_inverse)


def solution(mesh):
    sizes = tuple(mesh.shape[a] for a in AXES)
    placed = (P(None, "gx", "gy", "gz"), P("gx", "gy", "gz"), P(), P(), P())
    return jax.shard_map(
        functools.partial(on_device, sizes),
        mesh=mesh,
        in_specs=placed,
        out_specs=(P(None, "gx", "gy", "gz"), P(None, "gx", "gy", "gz")),
        check_vma=False,
    )
```
